32 devices in a mesh: groups: 2 (over x), replica: 16 (over z, y, core).
Axes of the slice: x: 2, y: 2, z: 4, core: 2. Of those that a mesh axis runs over, the one named last changes fastest.
Arguments:
- tokens: bfloat16 [32768, 2048], P(('groups', 'replica')), parts along dimension 0, may hold values from -6 to 6
- pseudo_keys: bfloat16 [32, 2048, 512], P(('groups', 'replica')), parts along dimension 0, may hold values from -0.875 to 0.875
- pseudo_values: bfloat16 [32, 2048, 512], P(('groups', 'replica')), parts along dimension 0, may hold values from -0.875 to 0.875
- master_keys: float32 [4096, 512], P(('groups', 'replica')), parts along dimension 0, may hold values from -0.125 to 0.125
- moment_keys: float32 [4096, 512], P(('groups', 'replica')), parts along dimension 0, may hold values from -0.125 to 0.125
- master_values: float32 [4096, 512], P(('groups', 'replica')), parts along dimension 0, may hold values from -0.125 to 0.125
- moment_values: float32 [4096, 512], P(('groups', 'replica')), parts along dimension 0, may hold values from -0.125 to 0.125
- outer_hyper: float32 [4], P('groups'), parts along dimension 0, may hold values from 0.5 to 0.95
Outputs:
- eval_keys: bfloat16 [32768, 512], P(('groups', 'replica')), parts along dimension 0
- eval_values: bfloat16 [32768, 512], P(('groups', 'replica')), parts along dimension 0
- new_master_keys: float32 [4096, 512], P(('groups', 'replica')), parts along dimension 0
- new_moment_keys: float32 [4096, 512], P(('groups', 'replica')), parts along dimension 0
- new_master_values: float32 [4096, 512], P(('groups', 'replica')), parts along dimension 0
- new_moment_values: float32 [4096, 512], P(('groups', 'replica')), parts along dimension 0
The draws below stay inside these ranges and needn't reach their ends.
There are 2 independent parts, one for each index of `groups`. The reference program is written for one: setup_inputs(seed, part) draws one part's arguments, and reference() takes and returns one part's arrays. A program takes and returns all parts, laid end to end along the dimension named above; each array names one. Nothing has to cross between parts.
All inputs are finite; a program needn't handle non-finite values.
Results may differ from the reference program's by a relative error of at most 0.0049.
Values may be sent and summed in bfloat16 or wider, within the bound.
A program may use at most 128 MiB of HBM per device.

```python
import jax
import jax.numpy as jnp

D = 2048
KVW = 512
TOKENS = 16384
N_REPLICA = 16


def with_spikes(array, stream_key, source, target, blocks, factor):
    owner, partner = [(jnp.arange(array.shape[position]) // (array.shape[position] // blocks)).reshape([-1 if axis == position else 1 for axis in range(array.ndim)]) for position in (source, target)]
    chosen = jax.random.permutation(stream_key, blocks)[partner]
    strong = (owner == chosen) | (owner == (partner + blocks // 2) % blocks)
    return jnp.where(strong, factor * array, array)


def levels(rng, shape, pieces, least, high):
    def one(dim, shards_of):
        heights = jax.random.uniform(jax.random.fold_in(jax.random.fold_in(rng, 6), dim), (shards_of,), jnp.float32, least / len(pieces), high / len(pieces))
        return jnp.repeat(jnp.exp(heights), shape[dim] // shards_of).reshape((-1,) + (1,) * (len(shape) - dim - 1))

    loudness = one(*pieces[0])
    for cut in pieces[1:]:
        loudness = loudness * one(*cut)
    return loudness


def gaussian(rng, dims, spread, limit, pieces=(), held_as=jnp.bfloat16):
    values = spread * jax.random.normal(rng, dims, jnp.float32)
    if pieces:
        values = values * levels(rng, dims, pieces, -0.22, 0.18)
    return jnp.clip(values, -limit, limit).astype(held_as)


def bell_draw_with(stream_key, dims, deviation, limit, pieces, heavy, dtype=jnp.bfloat16):
    drawn = deviation * jax.random.normal(stream_key, dims, jnp.float32)
    if pieces:
        drawn = drawn * levels(stream_key, dims, pieces, -0.22, 0.18)
    return jnp.clip(with_spikes(drawn, jax.random.fold_in(stream_key, 3), *heavy), -limit, limit).astype(dtype)


def setup_inputs(seed: int = 0, part: int = 0) -> dict:
    arg_keys = jax.random.split(jax.random.key(seed), 9)
    part_keys = jax.random.split(jax.random.fold_in(arg_keys[8], part), 9)
    return {
        "tokens": gaussian(part_keys[0], (TOKENS, D), 1.0, 6.0, ((0, 16),)),
        "pseudo_keys": bell_draw_with(part_keys[1], (N_REPLICA, D, KVW), 0.1, 0.875, ((0, 16),), (0, 1, 16, 2.0)),
        "pseudo_values": bell_draw_with(part_keys[2], (N_REPLICA, D, KVW), 0.1, 0.875, ((0, 16),), (0, 1, 16, 2.0)),
        "master_keys": gaussian(part_keys[3], (D, KVW), D ** -0.5, 0.125, ((0, 16),), jnp.float32),
        "moment_keys": gaussian(part_keys[4], (D, KVW), 0.02, 0.125, ((0, 16),), jnp.float32),
        "master_values": gaussian(part_keys[5], (D, KVW), D ** -0.5, 0.125, ((0, 16),), jnp.float32),
        "moment_values": gaussian(part_keys[6], (D, KVW), 0.02, 0.125, ((0, 16),), jnp.float32),
        "outer_hyper": jnp.clip(jax.random.uniform(part_keys[7], (2,), jnp.float32, 0.5, 0.95), 0.5, 0.95),
    }


def outer_update(pseudo, master, moment, outer_rate, outer_mom):
    averaged = jnp.sum(pseudo.astype(jnp.float32), axis=0) / N_REPLICA
    moment_new = outer_mom * moment + averaged
    master_new = master - outer_rate * (averaged + outer_mom * moment_new)
    return master_new, moment_new


def reference(tokens, pseudo_keys, pseudo_values, master_keys, moment_keys, master_values, moment_values, outer_hyper):
    outer_rate = outer_hyper[0]
    outer_mom = outer_hyper[1]
    master_k, moment_k = outer_update(pseudo_keys, master_keys, moment_keys, outer_rate, outer_mom)
    master_v, moment_v = outer_update(pseudo_values, master_values, moment_values, outer_rate, outer_mom)
    eval_keys = jnp.dot(tokens, master_k.astype(jnp.bfloat16), preferred_element_type=jnp.float32).astype(jnp.bfloat16)
    eval_values = jnp.dot(tokens, master_v.astype(jnp.bfloat16), preferred_element_type=jnp.float32).astype(jnp.bfloat16)
    return (eval_keys, eval_values, master_k, moment_k, master_v, moment_v)
```

```python
import functools

import jax
import jax.numpy as jnp
from jax import lax
from jax.experimental import pallas as pl
from jax.experimental.pallas import tpu as pltpu
from jax.sharding import PartitionSpec as P

MESH = pl.DeviceIdType.MESH
F32 = jnp.float32
BF16 = jnp.bfloat16

REDUCE = "ABAA"
GATHER = "AAAB"

TUNED = (
    ("Y", 0, 0), ("Y", 0, 1), ("Y", 0, 3), ("Z", 1, 0), ("Y", 2, 0), ("Y", 3, 0), ("Y", 2, 1), ("Y", 2, 2),
    ("Y", 3, 3), ("Y", 0, 2), ("Y", 2, 3), ("Y", 3, 1), ("Z", 0, 0), ("Z", 1, 1), ("Z", 1, 2), ("Z", 2, 0),
    ("Z", 3, 0), ("Z", 0, 1), ("Z", 0, 2), ("Z", 1, 3), ("Y", 3, 2), ("Z", 2, 1), ("Z", 3, 1), ("Z", 2, 2),
    ("Z", 0, 3), ("F", 0, 0), ("F", 1, 0), ("Z", 2, 3), ("F", 2, 0), ("Z", 3, 2), ("G", 0, 1), ("G", 1, 1),
    ("H", 2, 0), ("H", 0, 0), ("G", 2, 1), ("G", 1, 2), ("Z", 3, 3), ("F", 3, 0), ("D", 0, 0), ("D", 2, 0),
    ("H", 1, 0), ("G", 1, 3), ("G", 0, 2), ("H", 1, 1), ("D", 1, 0), ("G", 3, 1), ("H", 0, 1), ("G", 2, 2),
    ("H", 3, 0), ("H", 2, 1), ("G", 3, 2), ("D", 1, 1), ("D", 3, 0), ("G", 0, 3), ("D", 2, 1), ("H", 1, 3),
    ("H", 1, 2), ("D", 0, 1), ("G", 2, 3), ("H", 0, 2), ("K", 3, 1), ("D", 1, 2), ("D", 1, 3), ("H", 2, 2),
    ("K", 3, 2), ("D", 3, 1), ("G", 3, 3), ("H", 0, 3), ("D", 0, 2), ("D", 2, 2), ("H", 2, 3), ("D", 0, 3),
    ("K", 3, 3), ("D", 3, 2), ("D", 2, 3), ("D", 3, 3),
)


def plan(Z):
    steps = 1 + max(s for _, _, s in TUNED)
    if steps == Z:
        return TUNED
    units = range(len(REDUCE))
    order = [("Y", u, None) for u in units if REDUCE[u] == "A"]
    for u in units:
        order += [("Z", u, None), ("Z", u, Z - 1), ("F", u, 0)]
    for u in units:
        order += [("G", u, None)]
        order += [("H", u, None)] if GATHER[u] == "A" else [("H", u, 0), ("K", u, None)]
        order += [("D", u, 0), ("D", u, None), ("D", u, Z - 1)]
    return order


def kernel(
    Z,
    Y,
    replicas,
    tokens,
    pseudo_keys,
    pseudo_values,
    master_keys,
    moment_keys,
    master_values,
    moment_values,
    hyper_in,
    eval_keys,
    eval_values,
    out_master_keys,
    out_moment_keys,
    out_master_values,
    out_moment_values,
    tok,
    mine,
    from_core,
    to_y,
    from_y,
    to_z,
    from_left,
    from_right,
    weights,
    total,
    acc,
    master,
    moment,
    hyper,
    load_sem,
    state_sem,
    tok_sem,
    rc_s,
    rc_r,
    ry_s,
    ry_r,
    rz_s,
    rl_r,
    rr_r,
    gr_s,
    gl_s,
    gz_r,
    gy_s,
    gy_r,
    gc_s,
    gc_r,
):
    me = lax.axis_index("replica")
    core = lax.rem(me, 2)
    chip = lax.div(me, 2)
    y = lax.rem(chip, Y)
    z = lax.div(chip, Y)
    oc = 1 - core
    oy = 1 - y

    def dev(zz, yy, cc):
        return {"replica": (zz * Y + yy) * 2 + cc}

    pseudo = (pseudo_keys, pseudo_values)
    evals = (eval_keys, eval_values)
    states = ((out_master_keys, out_moment_keys), (out_master_values, out_moment_values))
    units = mine.shape[0]
    halves = units // 2
    rows, cols = mine.shape[3:]
    count = tok.shape[1]
    depth = tok.shape[2]

    def kv_of(u):
        return u // halves

    def lanes(u):
        return pl.ds((u % halves) * cols, cols)

    loads = [
        pltpu.make_async_copy(
            pseudo[kv_of(u)].at[:, :, core, :, lanes(u)], mine.at[u], load_sem.at[u]
        )
        for u in range(units)
    ]
    state_loads = [
        pltpu.make_async_copy(src, dst, state_sem.at[i])
        for i, (src, dst) in enumerate(
            (
                (master_keys, master.at[0]),
                (moment_keys, moment.at[0]),
                (master_values, master.at[1]),
                (moment_values, moment.at[1]),
                (hyper_in, hyper),
            )
        )
    ]
    if len(tokens.shape) == 3:
        tok_loads = [
            pltpu.make_async_copy(tokens.at[p], tok.at[p], tok_sem.at[p]) for p in range(Z)
        ]
    else:
        tok_loads = [
            pltpu.make_async_copy(
                tokens.at[:, p * depth : (p + 1) * depth], tok.at[p], tok_sem.at[p]
            )
            for p in range(Z)
        ]

    upper = 2 * z >= Z
    m = jnp.minimum(z, Z - 1 - z)

    def near(s):
        half = (s + 1) // 2 if isinstance(s, int) else lax.div(s + 1, 2)
        side = 2 * (s % 2) - 1 if isinstance(s, int) else 2 * lax.rem(s, 2) - 1
        place = jnp.where(s <= 2 * m, m + half * side, s)
        return jnp.where(upper, Z - 1 - place, place)

    def far(s):
        return near(Z - 1 - s)

    def remote(src, dst, send, recv, device):
        return pltpu.make_async_remote_copy(
            src_ref=src,
            dst_ref=dst,
            send_sem=send,
            recv_sem=recv,
            device_id=device,
            device_id_type=MESH,
        )

    def core_copy(u, p):
        return remote(
            pseudo[kv_of(u)].at[p, :, oc, :, lanes(u)],
            from_core.at[u, p],
            rc_s.at[u, p],
            rc_r.at[u, p],
            dev(z, y, oc),
        )

    def y_copy(u, p):
        return remote(
            to_y.at[u, p], from_y.at[u, p], ry_s.at[u, p], ry_r.at[u, p], dev(z, oy, core)
        )

    def z_refs(u, p):
        if REDUCE[u] == "A":
            return to_z.at[u, p, 0], from_left.at[u, p, 0], from_right.at[u, p, 0]
        return to_z.at[u, p], from_left.at[u, p], from_right.at[u, p]

    def right_copy(u, p):
        src, dst, _ = z_refs(u, p)
        return remote(src, dst, rz_s.at[u, p], rl_r.at[u, p], dev(z + 1, y, core))

    def left_copy(u, p):
        src, _, dst = z_refs(u, p)
        return remote(src, dst, rz_s.at[u, p], rr_r.at[u, p], dev(z - 1, y, core))

    def w_right(u, p, yy):
        w = weights.at[u, p, yy, core]
        return remote(w, w, gr_s.at[u, p, yy], gz_r.at[u, p, yy], dev(z + 1, y, core))

    def w_left(u, p, yy):
        w = weights.at[u, p, yy, core]
        return remote(w, w, gl_s.at[u, p, yy], gz_r.at[u, p, yy], dev(z - 1, y, core))

    def w_y(u, p, yy):
        w = weights.at[u, p, yy, core]
        return remote(w, w, gy_s.at[u, p], gy_r.at[u, p], dev(z, oy, core))

    def w_core(u, p, yy, cc):
        w = weights.at[u, p, yy, cc]
        return remote(w, w, gc_s.at[u, p, yy], gc_r.at[u, p, yy], dev(z, y, oc))

    for copy in loads:
        copy.start()

    barrier = pltpu.get_barrier_semaphore()
    pl.semaphore_signal(barrier, inc=1, device_id=dev(z, y, oc), device_id_type=MESH)
    pl.semaphore_signal(barrier, inc=1, device_id=dev(z, oy, core), device_id_type=MESH)

    @pl.when(z > 0)
    def _():
        pl.semaphore_signal(barrier, inc=1, device_id=dev(z - 1, y, core), device_id_type=MESH)

    @pl.when(z < Z - 1)
    def _():
        pl.semaphore_signal(barrier, inc=1, device_id=dev(z + 1, y, core), device_id_type=MESH)

    peers = 2 + jnp.where(z > 0, 1, 0) + jnp.where(z < Z - 1, 1, 0)
    pl.semaphore_wait(barrier, peers)

    def each(first, last, body):
        def run(s, carry):
            body(s)
            return carry

        lax.fori_loop(first, last, run, 0)

    for u in range(units):
        each(0, Z, lambda s: core_copy(u, far(s)).start())
    for copy in state_loads + tok_loads:
        copy.start()

    loaded = set()

    def once(name, copy):
        if name not in loaded:
            loaded.add(name)
            copy.wait()

    def pair_sum(u, p, *yy):
        index = (u, p) + yy
        return mine[index].astype(F32) + from_core[index].astype(F32)

    def reduce_y(u, s):
        p = far(s)
        core_copy(u, p).wait_recv()
        to_y[u, p] = pair_sum(u, p, oy).astype(BF16)
        y_copy(u, p).start()

    def reduce_z(u, s, last):
        p = far(s)
        first = REDUCE[u] == "A"
        if first:
            y_copy(u, p).wait_recv()
            part = total.at[u, y]
            part[...] = pair_sum(u, p, y) + from_y[u, p].astype(F32)
        else:
            core_copy(u, p).wait_recv()
            part = total.at[u]
            part[...] = pair_sum(u, p)
        out, left, right = z_refs(u, p)

        @pl.when((p >= z) & (z > 0))
        def _():
            right_copy(u, p).wait_recv()
            part[...] += left[...].astype(F32)

        @pl.when((p <= z) & (z < Z - 1))
        def _():
            left_copy(u, p).wait_recv()
            part[...] += right[...].astype(F32)

        if not last:
            out[...] = part[...].astype(BF16)

            @pl.when(p > z)
            def _():
                right_copy(u, p).start()

            @pl.when(p < z)
            def _():
                left_copy(u, p).start()
        elif not first:
            to_y[u, z] = total[u, oy].astype(BF16)
            y_copy(u, z).start()

    def spread(u, p, yy):
        @pl.when((p <= z) & (z < Z - 1))
        def _():
            w_right(u, p, yy).start()

        @pl.when((p >= z) & (z > 0))
        def _():
            w_left(u, p, yy).start()

    def update(u):
        kv, lane = kv_of(u), lanes(u)
        summed = total[u, y]
        if REDUCE[u] == "B":
            y_copy(u, z).wait_recv()
            summed += from_y[u, z].astype(F32)
        for i in (4, 2 * kv, 2 * kv + 1):
            once(("state", i), state_loads[i])
        outer_rate = hyper[0]
        outer_mom = hyper[1]
        averaged = summed / replicas
        moment_new = outer_mom * moment[kv, :, lane] + averaged
        master_new = master[kv, :, lane] - outer_rate * (averaged + outer_mom * moment_new)
        weights[u, z, y, core] = master_new.astype(BF16)
        if GATHER[u] == "A":
            spread(u, z, y)
            w_y(u, z, y).start()
        else:
            w_y(u, z, y).start()
            spread(u, z, y)
        w_core(u, z, y, core).start()
        master_out, moment_out = states[kv]
        master_out[:, lane] = master_new
        moment_out[:, lane] = moment_new

    def pass_z(u, s, yy):
        p = near(s)
        w_right(u, p, yy).wait_recv()
        spread(u, p, yy)
        if GATHER[u] == "A":
            w_y(u, p, yy).start()
        w_core(u, p, yy, core).start()

    def pass_y(u, s):
        p = near(s)
        w_y(u, p, oy).wait_recv()
        if GATHER[u] == "B":
            spread(u, p, oy)
        w_core(u, p, oy, core).start()

    tile = min(1024, count)

    def dot(u, s, place):
        p = near(s)
        for yy in range(Y):
            w_core(u, p, yy, oc).wait_recv()
        block = weights[u, p].reshape(2 * Y * rows, cols)

        def one(i):
            span = pl.ds(i * tile if isinstance(i, int) else pl.multiple_of(i * tile, tile), tile)
            part = jnp.dot(tok[p, span, :], block, preferred_element_type=F32)
            if place != "first":
                part += acc[u, span, :]
            if place == "last":
                evals[kv_of(u)][span, lanes(u)] = part.astype(BF16)
            else:
                acc[u, span, :] = part

        if count == tile:
            one(0)
        else:
            each(0, count // tile, one)

    def take(kind, u, s):
        if kind == "Y":
            once(("load", u), loads[u])
            if s is None:
                each(0, Z, lambda t: reduce_y(u, t))
            else:
                reduce_y(u, s)
        elif kind == "Z":
            once(("load", u), loads[u])
            if s is None:
                each(0, Z - 1, lambda t: reduce_z(u, t, False))
            else:
                reduce_z(u, s, s == Z - 1)
        elif kind == "F":
            update(u)
        elif kind in ("G", "K"):
            yy = y if kind == "G" else oy
            if s is None:
                each(1, Z, lambda t: pass_z(u, t, yy))
            else:
                pass_z(u, s, yy)
        elif kind == "H":
            if s is None:
                each(0, Z, lambda t: pass_y(u, t))
            else:
                pass_y(u, s)
        else:
            for i, copy in enumerate(tok_loads):
                once(("tokens", i), copy)
            if s is None:
                each(1, Z - 1, lambda t: dot(u, t, "middle"))
            else:
                dot(u, s, "first" if s == 0 else "last" if s == Z - 1 else "middle")

    for kind, u, s in plan(Z):
        take(kind, u, s)

    def sent(u, p, yy):
        @pl.when((p <= z) & (z < Z - 1))
        def _():
            w_right(u, p, yy).wait_send()

        @pl.when((p >= z) & (z > 0))
        def _():
            w_left(u, p, yy).wait_send()

    for u in range(units):

        def drain(p):
            core_copy(u, p).wait_send()
            if REDUCE[u] == "A":
                y_copy(u, p).wait_send()

            @pl.when(p != z)
            def _():
                right_copy(u, p).wait_send()

            sent(u, p, y)
            if GATHER[u] == "A":
                w_y(u, p, y).wait_send()
            else:
                sent(u, p, oy)
            w_core(u, p, y, core).wait_send()
            w_core(u, p, oy, core).wait_send()

        each(0, Z, drain)
        if REDUCE[u] == "B":
            y_copy(u, z).wait_send()
        if GATHER[u] == "B":
            w_y(u, z, y).wait_send()


def place(*refs):
    source, target, sem = refs[:6], refs[6:12], refs[12]
    stores = [pltpu.make_async_copy(source[i], target[i], sem.at[i]) for i in range(6)]
    for copy in stores:
        copy.start()
    for copy in stores:
        copy.wait()


def body(
    tokens,
    pseudo_keys,
    pseudo_values,
    master_keys,
    moment_keys,
    master_values,
    moment_values,
    outer_hyper,
):
    replicas = lax.axis_size("replica")
    Y = 2
    Z = replicas // (2 * Y)
    width = master_keys.shape[1]
    rows = master_keys.shape[0]
    count = tokens.shape[0]
    units = len(REDUCE)
    cols = 2 * width // units
    depth = 2 * Y * rows
    if depth % 128:
        tokens = tokens.reshape(count, Z, depth).swapaxes(0, 1)
    pseudo_keys, pseudo_values = (
        p.reshape(Z, Y, 2, rows, width) for p in (pseudo_keys, pseudo_values)
    )
    hbm = pl.BlockSpec(memory_space=pltpu.HBM)
    vmem = pl.BlockSpec(memory_space=pltpu.VMEM)
    dma = pltpu.SemaphoreType.DMA
    state = (master_keys.shape, F32)
    evaluated = ((count, width), BF16)
    shapes = (evaluated, evaluated, state, state, state, state)
    single = pltpu.VMEM((units, Z, rows, cols), BF16)
    double = pltpu.VMEM((units, Z, Y, rows, cols), BF16)
    results = pl.pallas_call(
        functools.partial(kernel, Z, Y, replicas),
        out_shape=tuple(pltpu.VMEM(*a) for a in shapes),
        in_specs=[hbm] * 8,
        out_specs=(vmem,) * 6,
        scratch_shapes=[
            pltpu.VMEM((Z, count, depth), BF16),
            double,
            double,
            single,
            single,
            double,
            double,
            double,
            pltpu.VMEM((units, Z, Y, 2, rows, cols), BF16),
            pltpu.VMEM((units, Y, rows, cols), F32),
            pltpu.VMEM((units, count, cols), F32),
            pltpu.VMEM((2, rows, width), F32),
            pltpu.VMEM((2, rows, width), F32),
            pltpu.SMEM((2,), F32),
            dma((units,)),
            dma((5,)),
            dma((Z,)),
            *[dma((units, Z))] * 7,
            *[dma((units, Z, Y))] * 3,
            *[dma((units, Z))] * 2,
            *[dma((units, Z, Y))] * 2,
        ],
        compiler_params=pltpu.CompilerParams(
            collective_id=0, has_side_effects=True, vmem_limit_bytes=50 * 1024 * 1024
        ),
        name="outer_step",
    )(
        *[
            pltpu.with_memory_space_constraint(a, pltpu.HBM)
            for a in (
                tokens,
                pseudo_keys,
                pseudo_values,
                master_keys,
                moment_keys,
                master_values,
                moment_values,
                outer_hyper,
            )
        ]
    )
    return pl.pallas_call(
        place,
        out_shape=tuple(jax.ShapeDtypeStruct(*a) for a in shapes),
        in_specs=[vmem] * 6,
        out_specs=(hbm,) * 6,
        scratch_shapes=[dma((6,))],
        name="place",
    )(*[pltpu.with_memory_space_constraint(r, pltpu.VMEM) for r in results])


def solution(mesh):
    rows = P(("groups", "replica"), None)
    stack = P(("groups", "replica"), None, None)
    return jax.shard_map(
        body,
        mesh=mesh,
        in_specs=(rows, stack, stack, rows, rows, rows, rows, P("groups")),
        out_specs=(rows,) * 6,
        check_vma=False,
    )
```

```python
import functools

import jax
import jax.numpy as jnp
from jax import lax
from jax.experimental import pallas as pl
from jax.experimental.pallas import tpu as pltpu
from jax.sharding import PartitionSpec as P

MESH = pl.DeviceIdType.MESH
F32 = jnp.float32
BF16 = jnp.bfloat16

UNITS = ((0, 0), (0, 1), (1, 0), (1, 1))
PARTS = (
    (0, 0, 6, "A", "A"),
    (0, 6, 8, "B", "A"),
    (1, 0, 6, "A", "A"),
    (1, 6, 8, "B", "B"),
    (2, 0, 6, "A", "A"),
    (2, 6, 8, "B", "B"),
    (3, 0, 6, "A", "A"),
    (3, 6, 8, "A", "B"),
)

BATCHES = ((0, 2, 0, 2), (0, 2, 2, 4), (2, 4, 0, 1), (2, 4, 1, 2), (2, 4, 2, 4))
TUNED = (
    ("C", 0, 0), ("Y", 0, 0), ("C", 0, 1), ("Y", 0, 1), ("C", 0, 2), ("Y", 0, 2), ("Z", 1, 0), ("C", 1, 0),
    ("Y", 2, 0), ("Z", 3, 0), ("C", 2, 0), ("Y", 4, 0), ("Z", 5, 0), ("C", 3, 0), ("Y", 6, 0), ("Y", 7, 0),
    ("Z", 1, 1), ("C", 2, 1), ("Y", 4, 1), ("C", 1, 2), ("Z", 3, 2), ("C", 3, 1), ("Y", 7, 1), ("Z", 1, 2),
    ("C", 1, 1), ("Y", 2, 1), ("C", 3, 2), ("Y", 7, 2), ("Y", 2, 2), ("Z", 3, 1), ("Y", 6, 2), ("C", 1, 3),
    ("Y", 2, 3), ("Y", 6, 1), ("Z", 5, 1), ("Z", 0, 0), ("C", 3, 3), ("Y", 7, 3), ("Z", 2, 0), ("Z", 4, 0),
    ("Z", 7, 0), ("Z", 6, 0), ("Z", 0, 1), ("Z", 2, 1), ("Z", 3, 3), ("C", 0, 3), ("Z", 1, 3), ("C", 2, 2),
    ("Z", 5, 2), ("Y", 0, 3), ("Y", 4, 2), ("Z", 2, 2), ("Z", 7, 1), ("Z", 0, 2), ("Z", 4, 1), ("Z", 6, 1),
    ("F", 3, 0), ("C", 2, 3), ("Z", 5, 3), ("Y", 6, 3), ("Z", 7, 2), ("F", 1, 0), ("Z", 2, 3), ("F", 2, 0),
    ("Z", 0, 3), ("F", 0, 0), ("G", 3, 1), ("Z", 6, 2), ("Z", 4, 2), ("F", 5, 0), ("Z", 7, 3), ("F", 7, 0),
    ("Y", 4, 3), ("G", 1, 1), ("G", 2, 1), ("G", 0, 1), ("H", 3, 0), ("H", 5, 0), ("H", 7, 0), ("Z", 6, 3),
    ("H", 0, 0), ("H", 2, 0), ("F", 6, 0), ("Z", 4, 3), ("F", 4, 0), ("G", 1, 2), ("K", 5, 1), ("G", 7, 1),
    ("H", 2, 1), ("G", 0, 2), ("G", 5, 1), ("H", 0, 1), ("G", 6, 1), ("G", 3, 2), ("G", 4, 1), ("G", 2, 2),
    ("G", 4, 2), ("H", 6, 0), ("G", 1, 3), ("H", 1, 1), ("H", 4, 0), ("H", 1, 0), ("G", 0, 3), ("K", 7, 1),
    ("G", 6, 2), ("K", 3, 1), ("G", 5, 2), ("D", 0, 0), ("G", 2, 3), ("K", 3, 2), ("D", 2, 0), ("K", 7, 2),
    ("G", 4, 3), ("H", 0, 2), ("H", 6, 1), ("K", 5, 2), ("G", 7, 2), ("H", 4, 1), ("G", 6, 3), ("D", 3, 0),
    ("K", 3, 3), ("G", 3, 3), ("H", 2, 2), ("H", 1, 2), ("G", 5, 3), ("H", 1, 3), ("K", 5, 3), ("H", 0, 3),
    ("K", 7, 3), ("H", 4, 2), ("G", 7, 3), ("H", 6, 2), ("H", 2, 3), ("D", 1, 0), ("H", 4, 3), ("H", 6, 3),
    ("D", 4, 0),
)


def plan(Z):
    if 1 + max(s for _, _, s in TUNED) == Z:
        return BATCHES, TUNED
    units, parts = range(len(UNITS)), range(len(PARTS))
    order = [("C", u, None) for u in units]
    order += [("Y", q, None) for q in parts if PARTS[q][3] == "A"]
    for q in parts:
        order += [("Z", q, None), ("Z", q, Z - 1), ("F", q, 0)]
    for q in parts:
        order += [("G", q, None)]
        order += [("H", q, None)] if PARTS[q][4] == "A" else [("H", q, 0), ("K", q, None)]
    return ((0, len(UNITS), 0, Z),), order + [("D", 0, 0)]


def offsets(sizes):
    return [sum(sizes[:i]) for i in range(len(sizes) + 1)]


def kernel(
    Z,
    Y,
    replicas,
    tokens,
    pseudo_keys,
    pseudo_values,
    master_keys,
    moment_keys,
    master_values,
    moment_values,
    hyper_in,
    evals,
    states,
    tok,
    mine,
    from_core,
    to_y,
    from_y,
    to_z,
    from_left,
    from_right,
    weights,
    total,
    acc,
    master,
    moment,
    hyper,
    load_sem,
    state_sem,
    tok_sem,
    rc_s,
    rc_r,
    sends,
    ry_r,
    z_r,
    gy_r,
    gc_r,
):
    me = lax.axis_index("replica")
    core = lax.rem(me, 2)
    chip = lax.div(me, 2)
    y = lax.rem(chip, Y)
    z = lax.div(chip, Y)
    oc = 1 - core
    oy = 1 - y

    def dev(zz, yy, cc):
        return {"replica": (zz * Y + yy) * 2 + cc}

    pseudo = (pseudo_keys, pseudo_values)
    units = len(UNITS)
    rows, cols = mine.shape[3:]
    count = acc.shape[1]
    depth = 2 * rows
    batches, order = plan(Z)

    def lanes(u):
        return pl.ds(UNITS[u][1] * cols, cols)

    def edge(eighths):
        return rows if eighths == 8 else rows * eighths // 8 // 16 * 16

    spans = [pl.ds(edge(first), edge(last) - edge(first)) for _, first, last, _, _ in PARTS]
    unit = [part[0] for part in PARTS]
    reduce = [part[3] for part in PARTS]
    gather = [part[4] for part in PARTS]
    used = [q for q in range(len(PARTS)) if spans[q].size]

    loads = [
        pltpu.make_async_copy(
            pseudo[kv].at[:, :, core, :, lanes(u)], mine.at[u], load_sem.at[u]
        )
        for u, (kv, _) in enumerate(UNITS)
    ]
    state_loads = [
        pltpu.make_async_copy(src, dst, state_sem.at[i])
        for i, (src, dst) in enumerate(
            (
                (master_keys, master.at[0]),
                (moment_keys, moment.at[0]),
                (master_values, master.at[1]),
                (moment_values, moment.at[1]),
                (hyper_in, hyper),
            )
        )
    ]
    tok_load = pltpu.make_async_copy(tokens, tok, tok_sem)

    reduce_y_at = offsets([Z if kind == "A" else 1 for kind in reduce])
    gather_y_at = offsets([Z if kind == "A" else 1 for kind in gather])
    second_at = offsets([1 if kind == "A" else Z for kind in gather])

    upper = 2 * z >= Z
    m = jnp.minimum(z, Z - 1 - z)

    def near(s):
        half = (s + 1) // 2 if isinstance(s, int) else lax.div(s + 1, 2)
        side = 2 * (s % 2) - 1 if isinstance(s, int) else 2 * lax.rem(s, 2) - 1
        place = jnp.where(s <= 2 * m, m + half * side, s)
        return jnp.where(upper, Z - 1 - place, place)

    def far(s):
        return near(Z - 1 - s)

    def remote(src, dst, send, recv, device):
        return pltpu.make_async_remote_copy(
            src_ref=src,
            dst_ref=dst,
            send_sem=send,
            recv_sem=recv,
            device_id=device,
            device_id_type=MESH,
        )

    def core_copy(u, p):
        return remote(
            pseudo[UNITS[u][0]].at[p, :, oc, :, lanes(u)],
            from_core.at[u, p],
            rc_s,
            rc_r.at[u, p],
            dev(z, y, oc),
        )

    def y_copy(q, p):
        index = (unit[q], p, spans[q])
        slot = reduce_y_at[q] + (p if reduce[q] == "A" else 0)
        return remote(
            to_y.at[index], from_y.at[index], sends.at[q], ry_r.at[slot], dev(z, oy, core)
        )

    def second(q, p):
        return len(PARTS) * Z + second_at[q] + (p if gather[q] == "B" else 0)

    def z_refs(q, p):
        index = (unit[q], p, 0 if reduce[q] == "A" else slice(None), spans[q])
        return to_z.at[index], from_left.at[index], from_right.at[index]

    def right_copy(q, p):
        src, dst, _ = z_refs(q, p)
        return remote(src, dst, sends.at[q], z_r.at[q * Z + p], dev(z + 1, y, core))

    def left_copy(q, p, to):
        src, _, dst = z_refs(q, p)
        slot = jnp.where(p == to, second(q, p), q * Z + p)
        return remote(src, dst, sends.at[q], z_r.at[slot], dev(z - 1, y, core))

    def block(q, p, yy, cc):
        return weights.at[((unit[q] * Z + p) * Y + yy) * 2 + cc, spans[q]]

    def w_z(q, p, col, zz):
        w = block(q, p, oy if col else y, core)
        slot = second(q, p) if col else q * Z + p
        return remote(w, w, sends.at[q], z_r.at[slot], dev(zz, y, core))

    def w_y(q, p, yy):
        w = block(q, p, yy, core)
        slot = gather_y_at[q] + (p if gather[q] == "A" else 0)
        return remote(w, w, sends.at[q], gy_r.at[slot], dev(z, oy, core))

    def w_core(q, p, yy):
        w = block(q, p, yy, core)
        return remote(w, w, sends.at[q], gc_r.at[unit[q] * Z + p], dev(z, y, oc))

    def each(first, last, body):
        def run(s, carry):
            body(s)
            return carry

        lax.fori_loop(first, last, run, 0)

    for copy in loads:
        copy.start()

    @functools.partial(each, 0, units)
    def _(u):
        @functools.partial(each, 0, count // 128)
        def _(i):
            acc[u, pl.ds(pl.multiple_of(i * 128, 128), 128), :] = jnp.zeros((128, cols), F32)

    barrier = pltpu.get_barrier_semaphore()
    pl.semaphore_signal(barrier, inc=1, device_id=dev(z, y, oc), device_id_type=MESH)
    pl.semaphore_signal(barrier, inc=1, device_id=dev(z, oy, core), device_id_type=MESH)

    @pl.when(z > 0)
    def _():
        pl.semaphore_signal(barrier, inc=1, device_id=dev(z - 1, y, core), device_id_type=MESH)

    @pl.when(z < Z - 1)
    def _():
        pl.semaphore_signal(barrier, inc=1, device_id=dev(z + 1, y, core), device_id_type=MESH)

    peers = 2 + jnp.where(z > 0, 1, 0) + jnp.where(z < Z - 1, 1, 0)
    pl.semaphore_wait(barrier, peers)

    for u in range(units):
        each(0, Z, lambda s: core_copy(u, far(s)).start())
    for copy in state_loads + [tok_load]:
        copy.start()

    loaded = set()

    def once(name, copy):
        if name not in loaded:
            loaded.add(name)
            copy.wait()

    def pair_sum(q, p, yy):
        index = (unit[q], p, yy, spans[q])
        return mine[index].astype(F32) + from_core[index].astype(F32)

    def reduce_y(q, s):
        p = far(s)
        to_y[unit[q], p, spans[q]] = pair_sum(q, p, oy).astype(BF16)
        y_copy(q, p).start()

    def reduce_z(q, s, last):
        p = far(s)
        u = unit[q]
        first = reduce[q] == "A"
        if first:
            y_copy(q, p).wait_recv()
            part = total.at[u, y, spans[q]]
            part[...] = pair_sum(q, p, y) + from_y[u, p, spans[q]].astype(F32)
        else:
            part = total.at[u, :, spans[q]]
            part[...] = pair_sum(q, p, slice(None))
        out, left, right = z_refs(q, p)

        @pl.when((p >= z) & (z > 0))
        def _():
            right_copy(q, p).wait_recv()
            part[...] += left[...].astype(F32)

        @pl.when((p <= z) & (z < Z - 1))
        def _():
            left_copy(q, p, z).wait_recv()
            part[...] += right[...].astype(F32)

        if not last:
            out[...] = part[...].astype(BF16)

            @pl.when(p > z)
            def _():
                right_copy(q, p).start()

            @pl.when(p < z)
            def _():
                left_copy(q, p, z - 1).start()
        elif not first:
            to_y[u, z, spans[q]] = total[u, oy, spans[q]].astype(BF16)
            y_copy(q, z).start()

    def spread(q, p, col):
        @pl.when((p < z) & (z < Z - 1))
        def _():
            w_z(q, p, col, z + 1).start()

        @pl.when((p > z) & (z > 0))
        def _():
            w_z(q, p, col, z - 1).start()

    def spread_own(q, col):
        @pl.when(z < Z - 1)
        def _():
            w_z(q, z, col, z + 1).start()

        @pl.when(z > 0)
        def _():
            w_z(q, z, col, z - 1).start()

    def update(q):
        u, span = unit[q], spans[q]
        kv, lane = UNITS[u][0], lanes(u)
        summed = total[u, y, span]
        if reduce[q] == "B":
            y_copy(q, z).wait_recv()
            summed += from_y[u, z, span].astype(F32)
        for i in (4, 2 * kv, 2 * kv + 1):
            once(("state", i), state_loads[i])
        outer_rate = hyper[0]
        outer_mom = hyper[1]
        averaged = summed / replicas
        moment_new = outer_mom * moment[kv, span, lane] + averaged
        master_new = master[kv, span, lane] - outer_rate * (averaged + outer_mom * moment_new)
        block(q, z, y, core)[...] = master_new.astype(BF16)
        if gather[q] == "A":
            spread_own(q, 0)
            w_y(q, z, y).start()
        else:
            w_y(q, z, y).start()
            spread_own(q, 0)
        w_core(q, z, y).start()
        states[2 * kv, span, lane] = master_new
        states[2 * kv + 1, span, lane] = moment_new

    def pass_z(q, s, col):
        p = near(s)
        w_z(q, p, col, z).wait_recv()
        spread(q, p, col)
        if gather[q] == "A":
            w_y(q, p, y).start()
        w_core(q, p, oy if col else y).start()

    def pass_y(q, s):
        p = near(s)
        w_y(q, p, oy).wait_recv()
        if gather[q] == "B":
            spread_own(q, 1)
        w_core(q, p, oy).start()

    tile = min(1024, count)

    def products(u0, u1, s0, s1):
        def one(t):
            u = u0 + lax.rem(t, u1 - u0)
            p = near(s0 + lax.div(t, u1 - u0))
            w = weights.at[:Y]
            remote(w, w, rc_s, gc_r.at[u * Z + p], dev(z, y, oc)).wait_recv()
            kv = lax.div(u, units // 2)
            lane = pl.ds(pl.multiple_of(lax.rem(u, units // 2) * cols, cols), cols)

            def strip(i):
                at = pl.ds(i * tile if isinstance(i, int) else pl.multiple_of(i * tile, tile), tile)
                part = acc[u, at, :]
                for yy in range(Y):
                    place = p * Y + yy
                    if len(tok.shape) == 3:
                        left = tok[place, at, :]
                    else:
                        left = tok[at, pl.ds(pl.multiple_of(place * depth, depth), depth)]
                    right = weights[pl.ds(((u * Z + p) * Y + yy) * 2, 2)].reshape(depth, cols)
                    part += jnp.dot(left, right, preferred_element_type=F32)
                acc[u, at, :] = part
                evals[kv, at, lane] = part.astype(BF16)

            if count == tile:
                strip(0)
            else:
                each(0, count // tile, strip)

        each(0, (u1 - u0) * (s1 - s0), one)

    def drain():
        remote(from_core, from_core, rc_s, rc_s, dev(z, y, oc)).wait_send()

        def sent(q, blocks):
            w = weights.at[:blocks, spans[q]]
            remote(w, w, sends.at[q], sends.at[q], dev(z, y, oc)).wait_send()

        for inner in (True, False):

            @pl.when(((z > 0) & (z < Z - 1)) == inner)
            def _():
                for q in used:
                    beside = Z + 1 if inner else 1
                    across = beside + Z if gather[q] == "A" else 2 * beside + 1
                    sent(q, 2 * Z - 1 + across + 2 * Z)

    def take(kind, i, s):
        if kind == "C":
            once(i, loads[i])
            if s is None:
                each(0, Z, lambda t: core_copy(i, far(t)).wait_recv())
            else:
                core_copy(i, far(s)).wait_recv()
        elif kind == "Y":
            if s is None:
                each(0, Z, lambda t: reduce_y(i, t))
            else:
                reduce_y(i, s)
        elif kind == "Z":
            if s is None:
                each(0, Z - 1, lambda t: reduce_z(i, t, False))
            else:
                reduce_z(i, s, s == Z - 1)
        elif kind == "F":
            update(i)
        elif kind in ("G", "K"):
            col = 0 if kind == "G" else 1
            if s is None:
                each(1, Z, lambda t: pass_z(i, t, col))
            else:
                pass_z(i, s, col)
        elif kind == "H":
            if s is None:
                each(0, Z, lambda t: pass_y(i, t))
            else:
                pass_y(i, s)
        else:
            once("tokens", tok_load)
            products(*batches[i])

    for kind, i, s in order:
        if kind in "CD" or i in used:
            take(kind, i, s)
    drain()


def place(evals, states, *refs):
    target, sem = refs[:6], refs[6]
    source = [evals.at[i] for i in range(2)] + [states.at[i] for i in range(4)]
    stores = [pltpu.make_async_copy(source[i], target[i], sem.at[i]) for i in range(6)]
    for copy in stores:
        copy.start()
    for copy in stores:
        copy.wait()


def body(
    tokens,
    pseudo_keys,
    pseudo_values,
    master_keys,
    moment_keys,
    master_values,
    moment_values,
    outer_hyper,
):
    replicas = lax.axis_size("replica")
    Y = 2
    Z = replicas // (2 * Y)
    width = master_keys.shape[1]
    rows = master_keys.shape[0]
    count = tokens.shape[0]
    units = len(UNITS)
    parts = len(PARTS)
    cols = 2 * width // units
    depth = 2 * rows
    if depth % 128:
        tokens = tokens.reshape(count, Z * Y, depth).swapaxes(0, 1)
    pseudo_keys, pseudo_values = (
        p.reshape(Z, Y, 2, rows, width) for p in (pseudo_keys, pseudo_values)
    )
    hbm = pl.BlockSpec(memory_space=pltpu.HBM)
    vmem = pl.BlockSpec(memory_space=pltpu.VMEM)
    dma = pltpu.SemaphoreType.DMA
    state = (master_keys.shape, F32)
    evaluated = ((count, width), BF16)
    shapes = (evaluated, evaluated, state, state, state, state)
    single = pltpu.VMEM((units, Z, rows, cols), BF16)
    double = pltpu.VMEM((units, Z, Y, rows, cols), BF16)
    results = pl.pallas_call(
        functools.partial(kernel, Z, Y, replicas),
        out_shape=(pltpu.VMEM((2, count, width), BF16), pltpu.VMEM((4, rows, width), F32)),
        in_specs=[hbm] * 8,
        out_specs=(vmem,) * 2,
        scratch_shapes=[
            pltpu.VMEM(tokens.shape, BF16),
            double,
            double,
            single,
            single,
            double,
            double,
            double,
            pltpu.VMEM((units * Z * Y * 2, rows, cols), BF16),
            pltpu.VMEM((units, Y, rows, cols), F32),
            pltpu.VMEM((units, count, cols), F32),
            pltpu.VMEM((2, rows, width), F32),
            pltpu.VMEM((2, rows, width), F32),
            pltpu.SMEM((2,), F32),
            dma((units,)),
            dma((5,)),
            dma,
            dma,
            dma((units, Z)),
            dma((parts,)),
            dma((sum(Z if part[3] == "A" else 1 for part in PARTS),)),
            dma((parts * Z + sum(1 if part[4] == "A" else Z for part in PARTS),)),
            dma((sum(Z if part[4] == "A" else 1 for part in PARTS),)),
            dma((units * Z,)),
        ],
        compiler_params=pltpu.CompilerParams(
            collective_id=0, has_side_effects=True, vmem_limit_bytes=50 * 1024 * 1024
        ),
        name="outer_step",
    )(
        *[
            pltpu.with_memory_space_constraint(a, pltpu.HBM)
            for a in (
                tokens,
                pseudo_keys,
                pseudo_values,
                master_keys,
                moment_keys,
                master_values,
                moment_values,
                outer_hyper,
            )
        ]
    )
    return pl.pallas_call(
        place,
        out_shape=tuple(jax.ShapeDtypeStruct(*a) for a in shapes),
        in_specs=[vmem] * 2,
        out_specs=(hbm,) * 6,
        scratch_shapes=[dma((6,))],
        name="place",
    )(*[pltpu.with_memory_space_constraint(r, pltpu.VMEM) for r in results])


def solution(mesh):
    rows = P(("groups", "replica"), None)
    stack = P(("groups", "replica"), None, None)
    return jax.shard_map(
        body,
        mesh=mesh,
        in_specs=(rows, stack, stack, rows, rows, rows, rows, P("groups")),
        out_specs=(rows,) * 6,
        check_vma=False,
    )
```

```python
import functools

import jax
import jax.numpy as jnp
from jax import lax
from jax.experimental import pallas as pl
from jax.experimental.pallas import tpu as pltpu
from jax.sharding import PartitionSpec as P

MESH = pl.DeviceIdType.MESH
F32 = jnp.float32
BF16 = jnp.bfloat16

UNITS = ((0, 0), (0, 1), (1, 0), (1, 1))
PARTS = (
    (0, 0, 6, "A", "A"),
    (0, 6, 8, "B", "A"),
    (1, 0, 6, "A", "A"),
    (1, 6, 8, "B", "B"),
    (2, 0, 6, "A", "A"),
    (2, 6, 8, "B", "B"),
    (3, 0, 6, "A", "A"),
    (3, 6, 8, "A", "B"),
)

BATCHES = ((0, 2, 0, 1), (0, 2, 1, 2), (0, 2, 2, 3), (0, 2, 3, 4), (2, 4, 0, 1), (2, 4, 1, 2), (2, 4, 2, 3), (2, 4, 3, 4))
TUNED = (
    ("C", 0, 0), ("Y", 0, 0), ("C", 0, 1), ("Y", 0, 1), ("C", 0, 2), ("Y", 0, 2), ("Z", 1, 0), ("C", 1, 0),
    ("Y", 2, 0), ("Z", 3, 0), ("C", 2, 0), ("Y", 4, 0), ("Z", 5, 0), ("C", 3, 0), ("Y", 6, 0), ("Y", 7, 0),
    ("C", 1, 1), ("Y", 2, 1), ("Z", 3, 1), ("C", 2, 2), ("Y", 4, 2), ("C", 3, 1), ("Y", 7, 1), ("C", 1, 2),
    ("Z", 3, 2), ("Z", 0, 0), ("Z", 1, 1), ("Z", 1, 2), ("C", 2, 1), ("Y", 4, 1), ("Z", 2, 0), ("C", 3, 2),
    ("Y", 7, 2), ("Y", 2, 2), ("Z", 4, 0), ("Y", 6, 1), ("Z", 6, 0), ("Z", 7, 0), ("Z", 5, 1), ("C", 0, 3),
    ("Y", 0, 3), ("Z", 0, 1), ("Z", 1, 3), ("Z", 2, 1), ("Z", 5, 2), ("C", 1, 3), ("Z", 3, 3), ("Z", 4, 1),
    ("Z", 0, 2), ("Y", 2, 3), ("Y", 6, 2), ("Z", 2, 2), ("Z", 7, 1), ("C", 2, 3), ("Z", 5, 3), ("Z", 6, 1),
    ("F", 1, 0), ("F", 3, 0), ("Z", 4, 2), ("Y", 4, 3), ("Z", 0, 3), ("F", 0, 0), ("C", 3, 3), ("Y", 6, 3),
    ("G", 1, 1), ("Z", 2, 3), ("G", 3, 1), ("F", 5, 0), ("Z", 7, 2), ("Y", 7, 3), ("Z", 6, 2), ("H", 3, 0),
    ("F", 2, 0), ("G", 0, 1), ("Z", 4, 3), ("F", 4, 0), ("G", 1, 2), ("G", 5, 1), ("H", 5, 0), ("Z", 7, 3),
    ("F", 7, 0), ("Z", 6, 3), ("K", 3, 1), ("H", 1, 0), ("F", 6, 0), ("G", 0, 2), ("H", 2, 0), ("G", 2, 1),
    ("G", 3, 2), ("G", 4, 1), ("G", 5, 2), ("H", 1, 1), ("K", 3, 2), ("G", 6, 1), ("H", 7, 0), ("G", 7, 1),
    ("G", 2, 2), ("H", 0, 0), ("H", 6, 0), ("K", 5, 1), ("G", 4, 2), ("H", 4, 0), ("G", 6, 2), ("K", 5, 2),
    ("G", 0, 3), ("G", 1, 3), ("G", 7, 2), ("H", 0, 2), ("D", 4, 0), ("K", 7, 1), ("H", 0, 1), ("H", 1, 2),
    ("G", 2, 3), ("H", 2, 1), ("K", 7, 2), ("H", 4, 1), ("D", 0, 0), ("G", 4, 3), ("H", 6, 1), ("D", 1, 0),
    ("G", 6, 3), ("H", 2, 2), ("D", 5, 0), ("K", 7, 3), ("H", 4, 2), ("G", 3, 3), ("D", 2, 0), ("H", 6, 2),
    ("K", 3, 3), ("G", 5, 3), ("G", 7, 3), ("H", 0, 3), ("K", 5, 3), ("H", 2, 3), ("H", 1, 3), ("H", 4, 3),
    ("D", 6, 0), ("H", 6, 3), ("D", 3, 0), ("D", 7, 0),
)


def plan(Z):
    if 1 + max(s for _, _, s in TUNED) == Z:
        return BATCHES, TUNED
    units, parts = range(len(UNITS)), range(len(PARTS))
    order = [("C", u, None) for u in units]
    order += [("Y", q, None) for q in parts if PARTS[q][3] == "A"]
    for q in parts:
        order += [("Z", q, None), ("Z", q, Z - 1), ("F", q, 0)]
    for q in parts:
        order += [("G", q, None)]
        order += [("H", q, None)] if PARTS[q][4] == "A" else [("H", q, 0), ("K", q, None)]
    return ((0, len(UNITS), 0, Z),), order + [("D", 0, 0)]


def offsets(sizes):
    return [sum(sizes[:i]) for i in range(len(sizes) + 1)]


def kernel(
    Z,
    Y,
    replicas,
    tokens,
    pseudo_keys,
    pseudo_values,
    master_keys,
    moment_keys,
    master_values,
    moment_values,
    hyper_in,
    evals,
    states,
    tok,
    mine,
    from_core,
    to_y,
    from_y,
    to_z,
    from_left,
    from_right,
    weights,
    total,
    acc,
    master,
    moment,
    hyper,
    load_sem,
    state_sem,
    tok_sem,
    rc_s,
    rc_r,
    sends,
    ry_r,
    z_r,
    gy_r,
    gc_r,
):
    me = lax.axis_index("replica")
    core = lax.rem(me, 2)
    chip = lax.div(me, 2)
    y = lax.rem(chip, Y)
    z = lax.div(chip, Y)
    oc = 1 - core
    oy = 1 - y

    def dev(zz, yy, cc):
        return {"replica": (zz * Y + yy) * 2 + cc}

    pseudo = (pseudo_keys, pseudo_values)
    units = len(UNITS)
    rows, cols = mine.shape[3:]
    count = acc.shape[1]
    depth = 2 * Y * rows
    batches, order = plan(Z)

    def lanes(u):
        return pl.ds(UNITS[u][1] * cols, cols)

    def edge(eighths):
        return rows if eighths == 8 else rows * eighths // 8 // 16 * 16

    spans = [pl.ds(edge(first), edge(last) - edge(first)) for _, first, last, _, _ in PARTS]
    unit = [part[0] for part in PARTS]
    reduce = [part[3] for part in PARTS]
    gather = [part[4] for part in PARTS]
    used = [q for q in range(len(PARTS)) if spans[q].size]

    loads = [
        pltpu.make_async_copy(
            pseudo[kv].at[:, :, core, :, lanes(u)], mine.at[u], load_sem.at[u]
        )
        for u, (kv, _) in enumerate(UNITS)
    ]
    state_loads = [
        pltpu.make_async_copy(src, dst, state_sem.at[i])
        for i, (src, dst) in enumerate(
            (
                (master_keys, master.at[0]),
                (moment_keys, moment.at[0]),
                (master_values, master.at[1]),
                (moment_values, moment.at[1]),
                (hyper_in, hyper),
            )
        )
    ]
    tok_load = pltpu.make_async_copy(tokens, tok, tok_sem)

    reduce_y_at = offsets([Z if kind == "A" else 1 for kind in reduce])
    gather_y_at = offsets([Z if kind == "A" else 1 for kind in gather])
    second_at = offsets([1 if kind == "A" else Z for kind in gather])

    upper = 2 * z >= Z
    m = jnp.minimum(z, Z - 1 - z)

    def near(s):
        half = (s + 1) // 2 if isinstance(s, int) else lax.div(s + 1, 2)
        side = 2 * (s % 2) - 1 if isinstance(s, int) else 2 * lax.rem(s, 2) - 1
        place = jnp.where(s <= 2 * m, m + half * side, s)
        return jnp.where(upper, Z - 1 - place, place)

    def far(s):
        return near(Z - 1 - s)

    def remote(src, dst, send, recv, device):
        return pltpu.make_async_remote_copy(
            src_ref=src,
            dst_ref=dst,
            send_sem=send,
            recv_sem=recv,
            device_id=device,
            device_id_type=MESH,
        )

    def core_copy(u, p):
        return remote(
            pseudo[UNITS[u][0]].at[p, :, oc, :, lanes(u)],
            from_core.at[u, p],
            rc_s,
            rc_r.at[u, p],
            dev(z, y, oc),
        )

    def y_copy(q, p):
        index = (unit[q], p, spans[q])
        slot = reduce_y_at[q] + (p if reduce[q] == "A" else 0)
        return remote(
            to_y.at[index], from_y.at[index], sends.at[q], ry_r.at[slot], dev(z, oy, core)
        )

    def second(q, p):
        return len(PARTS) * Z + second_at[q] + (p if gather[q] == "B" else 0)

    def z_refs(q, p):
        index = (unit[q], p, 0 if reduce[q] == "A" else slice(None), spans[q])
        return to_z.at[index], from_left.at[index], from_right.at[index]

    def right_copy(q, p):
        src, dst, _ = z_refs(q, p)
        return remote(src, dst, sends.at[q], z_r.at[q * Z + p], dev(z + 1, y, core))

    def left_copy(q, p, to):
        src, _, dst = z_refs(q, p)
        slot = jnp.where(p == to, second(q, p), q * Z + p)
        return remote(src, dst, sends.at[q], z_r.at[slot], dev(z - 1, y, core))

    def block(q, p, yy, cc):
        return weights.at[((unit[q] * Z + p) * Y + yy) * 2 + cc, spans[q]]

    def w_z(q, p, col, zz):
        w = block(q, p, oy if col else y, core)
        slot = second(q, p) if col else q * Z + p
        return remote(w, w, sends.at[q], z_r.at[slot], dev(zz, y, core))

    def w_y(q, p, yy):
        w = block(q, p, yy, core)
        slot = gather_y_at[q] + (p if gather[q] == "A" else 0)
        return remote(w, w, sends.at[q], gy_r.at[slot], dev(z, oy, core))

    def w_core(q, p, yy):
        w = block(q, p, yy, core)
        return remote(w, w, sends.at[q], gc_r.at[unit[q] * Z + p], dev(z, y, oc))

    def each(first, last, body):
        def run(s, carry):
            body(s)
            return carry

        lax.fori_loop(first, last, run, 0)

    for copy in loads:
        copy.start()

    @functools.partial(each, 0, units)
    def _(u):
        @functools.partial(each, 0, count // 128)
        def _(i):
            acc[u, pl.ds(pl.multiple_of(i * 128, 128), 128), :] = jnp.zeros((128, cols), F32)

    barrier = pltpu.get_barrier_semaphore()
    pl.semaphore_signal(barrier, inc=1, device_id=dev(z, y, oc), device_id_type=MESH)
    pl.semaphore_signal(barrier, inc=1, device_id=dev(z, oy, core), device_id_type=MESH)

    @pl.when(z > 0)
    def _():
        pl.semaphore_signal(barrier, inc=1, device_id=dev(z - 1, y, core), device_id_type=MESH)

    @pl.when(z < Z - 1)
    def _():
        pl.semaphore_signal(barrier, inc=1, device_id=dev(z + 1, y, core), device_id_type=MESH)

    peers = 2 + jnp.where(z > 0, 1, 0) + jnp.where(z < Z - 1, 1, 0)
    pl.semaphore_wait(barrier, peers)

    for u in range(units):
        each(0, Z, lambda s: core_copy(u, far(s)).start())
    for copy in state_loads + [tok_load]:
        copy.start()

    loaded = set()

    def once(name, copy):
        if name not in loaded:
            loaded.add(name)
            copy.wait()

    def pair_sum(q, p, yy):
        index = (unit[q], p, yy, spans[q])
        return mine[index].astype(F32) + from_core[index].astype(F32)

    def reduce_y(q, s):
        p = far(s)
        to_y[unit[q], p, spans[q]] = pair_sum(q, p, oy).astype(BF16)
        y_copy(q, p).start()

    def reduce_z(q, s, last):
        p = far(s)
        u = unit[q]
        first = reduce[q] == "A"
        if first:
            y_copy(q, p).wait_recv()
            part = total.at[u, y, spans[q]]
            part[...] = pair_sum(q, p, y) + from_y[u, p, spans[q]].astype(F32)
        else:
            part = total.at[u, :, spans[q]]
            part[...] = pair_sum(q, p, slice(None))
        out, left, right = z_refs(q, p)

        @pl.when((p >= z) & (z > 0))
        def _():
            right_copy(q, p).wait_recv()
            part[...] += left[...].astype(F32)

        @pl.when((p <= z) & (z < Z - 1))
        def _():
            left_copy(q, p, z).wait_recv()
            part[...] += right[...].astype(F32)

        if not last:
            out[...] = part[...].astype(BF16)

            @pl.when(p > z)
            def _():
                right_copy(q, p).start()

            @pl.when(p < z)
            def _():
                left_copy(q, p, z - 1).start()
        elif not first:
            to_y[u, z, spans[q]] = total[u, oy, spans[q]].astype(BF16)
            y_copy(q, z).start()

    def spread(q, p, col):
        @pl.when((p < z) & (z < Z - 1))
        def _():
            w_z(q, p, col, z + 1).start()

        @pl.when((p > z) & (z > 0))
        def _():
            w_z(q, p, col, z - 1).start()

    def spread_own(q, col):
        @pl.when(z < Z - 1)
        def _():
            w_z(q, z, col, z + 1).start()

        @pl.when(z > 0)
        def _():
            w_z(q, z, col, z - 1).start()

    def update(q):
        u, span = unit[q], spans[q]
        kv, lane = UNITS[u][0], lanes(u)
        summed = total[u, y, span]
        if reduce[q] == "B":
            y_copy(q, z).wait_recv()
            summed += from_y[u, z, span].astype(F32)
        for i in (4, 2 * kv, 2 * kv + 1):
            once(("state", i), state_loads[i])
        outer_rate = hyper[0]
        outer_mom = hyper[1]
        averaged = summed / replicas
        moment_new = outer_mom * moment[kv, span, lane] + averaged
        master_new = master[kv, span, lane] - outer_rate * (averaged + outer_mom * moment_new)
        block(q, z, y, core)[...] = master_new.astype(BF16)
        if gather[q] == "A":
            spread_own(q, 0)
            w_y(q, z, y).start()
        else:
            w_y(q, z, y).start()
            spread_own(q, 0)
        w_core(q, z, y).start()
        states[2 * kv, span, lane] = master_new
        states[2 * kv + 1, span, lane] = moment_new

    def pass_z(q, s, col):
        p = near(s)
        w_z(q, p, col, z).wait_recv()
        spread(q, p, col)
        if gather[q] == "A":
            w_y(q, p, y).start()
        w_core(q, p, oy if col else y).start()

    def pass_y(q, s):
        p = near(s)
        w_y(q, p, oy).wait_recv()
        if gather[q] == "B":
            spread_own(q, 1)
        w_core(q, p, oy).start()

    tile = min(1024, count)

    def products(u0, u1, s0, s1):
        def one(t):
            p = near(s0 + t)
            for u in range(u0, u1):
                w = weights.at[:Y]
                remote(w, w, rc_s, gc_r.at[u * Z + p], dev(z, y, oc)).wait_recv()

            def strip(i):
                at = pl.ds(i * tile if isinstance(i, int) else pl.multiple_of(i * tile, tile), tile)
                if len(tok.shape) == 3:
                    left = tok[p, at, :]
                else:
                    left = tok[at, pl.ds(pl.multiple_of(p * depth, depth), depth)]
                for u in range(u0, u1):
                    right = weights[pl.ds((u * Z + p) * 2 * Y, 2 * Y)].reshape(depth, cols)
                    part = acc[u, at, :] + jnp.dot(left, right, preferred_element_type=F32)
                    acc[u, at, :] = part
                    evals[UNITS[u][0], at, lanes(u)] = part.astype(BF16)

            if count == tile:
                strip(0)
            else:
                each(0, count // tile, strip)

        each(0, s1 - s0, one)

    def drain():
        remote(from_core, from_core, rc_s, rc_s, dev(z, y, oc)).wait_send()

        def sent(q, blocks):
            w = weights.at[:blocks, spans[q]]
            remote(w, w, sends.at[q], sends.at[q], dev(z, y, oc)).wait_send()

        for inner in (True, False):

            @pl.when(((z > 0) & (z < Z - 1)) == inner)
            def _():
                for q in used:
                    beside = Z + 1 if inner else 1
                    across = beside + Z if gather[q] == "A" else 2 * beside + 1
                    sent(q, 2 * Z - 1 + across + 2 * Z)

    def take(kind, i, s):
        if kind == "C":
            once(i, loads[i])
            if s is None:
                each(0, Z, lambda t: core_copy(i, far(t)).wait_recv())
            else:
                core_copy(i, far(s)).wait_recv()
        elif kind == "Y":
            if s is None:
                each(0, Z, lambda t: reduce_y(i, t))
            else:
                reduce_y(i, s)
        elif kind == "Z":
            if s is None:
                each(0, Z - 1, lambda t: reduce_z(i, t, False))
            else:
                reduce_z(i, s, s == Z - 1)
        elif kind == "F":
            update(i)
        elif kind in ("G", "K"):
            col = 0 if kind == "G" else 1
            if s is None:
                each(1, Z, lambda t: pass_z(i, t, col))
            else:
                pass_z(i, s, col)
        elif kind == "H":
            if s is None:
                each(0, Z, lambda t: pass_y(i, t))
            else:
                pass_y(i, s)
        else:
            once("tokens", tok_load)
            products(*batches[i])

    for kind, i, s in order:
        if kind in "CD" or i in used:
            take(kind, i, s)
    drain()


def place(evals, states, *refs):
    target, sem = refs[:6], refs[6]
    source = [evals.at[i] for i in range(2)] + [states.at[i] for i in range(4)]
    stores = [pltpu.make_async_copy(source[i], target[i], sem.at[i]) for i in range(6)]
    for copy in stores:
        copy.start()
    for copy in stores:
        copy.wait()


def body(
    tokens,
    pseudo_keys,
    pseudo_values,
    master_keys,
    moment_keys,
    master_values,
    moment_values,
    outer_hyper,
):
    replicas = lax.axis_size("replica")
    Y = 2
    Z = replicas // (2 * Y)
    width = master_keys.shape[1]
    rows = master_keys.shape[0]
    count = tokens.shape[0]
    units = len(UNITS)
    parts = len(PARTS)
    cols = 2 * width // units
    depth = 2 * Y * rows
    if depth % 128:
        tokens = tokens.reshape(count, Z, depth).swapaxes(0, 1)
    pseudo_keys, pseudo_values = (
        p.reshape(Z, Y, 2, rows, width) for p in (pseudo_keys, pseudo_values)
    )
    hbm = pl.BlockSpec(memory_space=pltpu.HBM)
    vmem = pl.BlockSpec(memory_space=pltpu.VMEM)
    dma = pltpu.SemaphoreType.DMA
    state = (master_keys.shape, F32)
    evaluated = ((count, width), BF16)
    shapes = (evaluated, evaluated, state, state, state, state)
    single = pltpu.VMEM((units, Z, rows, cols), BF16)
    double = pltpu.VMEM((units, Z, Y, rows, cols), BF16)
    results = pl.pallas_call(
        functools.partial(kernel, Z, Y, replicas),
        out_shape=(pltpu.VMEM((2, count, width), BF16), pltpu.VMEM((4, rows, width), F32)),
        in_specs=[hbm] * 8,
        out_specs=(vmem,) * 2,
        scratch_shapes=[
            pltpu.VMEM(tokens.shape, BF16),
            double,
            double,
            single,
            single,
            double,
            double,
            double,
            pltpu.VMEM((units * Z * Y * 2, rows, cols), BF16),
            pltpu.VMEM((units, Y, rows, cols), F32),
            pltpu.VMEM((units, count, cols), F32),
            pltpu.VMEM((2, rows, width), F32),
            pltpu.VMEM((2, rows, width), F32),
            pltpu.SMEM((2,), F32),
            dma((units,)),
            dma((5,)),
            dma,
            dma,
            dma((units, Z)),
            dma((parts,)),
            dma((sum(Z if part[3] == "A" else 1 for part in PARTS),)),
            dma((parts * Z + sum(1 if part[4] == "A" else Z for part in PARTS),)),
            dma((sum(Z if part[4] == "A" else 1 for part in PARTS),)),
            dma((units * Z,)),
        ],
        compiler_params=pltpu.CompilerParams(
            collective_id=0, has_side_effects=True, vmem_limit_bytes=50 * 1024 * 1024
        ),
        name="outer_step",
    )(
        *[
            pltpu.with_memory_space_constraint(a, pltpu.HBM)
            for a in (
                tokens,
                pseudo_keys,
                pseudo_values,
                master_keys,
                moment_keys,
                master_values,
                moment_values,
                outer_hyper,
            )
        ]
    )
    return pl.pallas_call(
        place,
        out_shape=tuple(jax.ShapeDtypeStruct(*a) for a in shapes),
        in_specs=[vmem] * 2,
        out_specs=(hbm,) * 6,
        scratch_shapes=[dma((6,))],
        name="place",
    )(*[pltpu.with_memory_space_constraint(r, pltpu.VMEM) for r in results])


def solution(mesh):
    rows = P(("groups", "replica"), None)
    stack = P(("groups", "replica"), None, None)
    return jax.shard_map(
        body,
        mesh=mesh,
        in_specs=(rows, stack, stack, rows, rows, rows, rows, P("groups")),
        out_specs=(rows,) * 6,
        check_vma=False,
    )
```

```python
import functools

import jax
import jax.numpy as jnp
from jax import lax
from jax.experimental import pallas as pl
from jax.experimental.pallas import tpu as pltpu
from jax.sharding import PartitionSpec as P

MESH = pl.DeviceIdType.MESH
F32 = jnp.float32
BF16 = jnp.bfloat16

UNITS = ((0, 0), (0, 1), (1, 0), (1, 1))
PARTS = (
    (0, 0, 6, "A", "A"),
    (0, 6, 8, "B", "A"),
    (1, 0, 6, "A", "A"),
    (1, 6, 8, "B", "B"),
    (2, 0, 6, "A", "A"),
    (2, 6, 8, "B", "B"),
    (3, 0, 6, "A", "A"),
    (3, 6, 8, "A", "B"),
)

BATCHES = ((0, 0, 1), (0, 1, 2), (0, 2, 3), (0, 3, 4), (1, 0, 1), (1, 1, 2), (1, 2, 3), (1, 3, 4))
TUNED = (
    ("C", 0, 0), ("Y", 0, 0), ("C", 0, 3), ("Y", 0, 3), ("C", 1, 0), ("Y", 2, 0), ("C", 0, 1), ("Y", 0, 1),
    ("Z", 3, 0), ("C", 2, 0), ("Y", 4, 0), ("Z", 1, 0), ("C", 3, 0), ("Y", 6, 0), ("Z", 5, 0), ("C", 1, 2),
    ("Y", 2, 2), ("Y", 7, 0), ("C", 1, 1), ("Z", 3, 1), ("C", 3, 1), ("Y", 7, 1), ("C", 0, 2), ("Y", 0, 2),
    ("Y", 2, 1), ("C", 2, 1), ("Y", 4, 1), ("Z", 0, 0), ("Z", 1, 1), ("Z", 3, 2), ("Z", 1, 2), ("Z", 2, 0),
    ("C", 3, 3), ("Y", 6, 3), ("Z", 4, 0), ("Y", 6, 1), ("Z", 6, 0), ("Z", 5, 1), ("C", 1, 3), ("Z", 3, 3),
    ("C", 2, 2), ("Y", 4, 2), ("Z", 7, 0), ("Y", 2, 3), ("Z", 0, 1), ("Z", 5, 2), ("Z", 2, 1), ("Z", 1, 3),
    ("C", 3, 2), ("Y", 6, 2), ("Z", 4, 1), ("Z", 0, 2), ("Z", 6, 1), ("Z", 2, 2), ("Z", 7, 1), ("F", 3, 0),
    ("C", 2, 3), ("Z", 5, 3), ("Y", 7, 2), ("Y", 4, 3), ("Z", 4, 2), ("F", 1, 0), ("Z", 0, 3), ("F", 0, 0),
    ("Z", 6, 2), ("H", 3, 0), ("Y", 7, 3), ("F", 5, 0), ("Z", 2, 3), ("G", 3, 1), ("Z", 7, 2), ("F", 2, 0),
    ("G", 1, 1), ("Z", 4, 3), ("F", 4, 0), ("G", 0, 1), ("G", 1, 2), ("H", 5, 0), ("Z", 6, 3), ("F", 6, 0),
    ("H", 0, 0), ("Z", 7, 3), ("F", 7, 0), ("G", 2, 1), ("G", 0, 2), ("G", 4, 1), ("G", 2, 2), ("H", 1, 0),
    ("G", 5, 1), ("H", 0, 1), ("K", 5, 1), ("H", 6, 0), ("H", 2, 0), ("G", 6, 1), ("G", 4, 2), ("H", 7, 0),
    ("G", 6, 2), ("K", 5, 2), ("G", 5, 2), ("H", 1, 1), ("H", 1, 2), ("G", 1, 3), ("G", 0, 3), ("H", 4, 0),
    ("D", 0, 0), ("G", 3, 2), ("G", 2, 3), ("D", 4, 0), ("H", 2, 1), ("K", 3, 2), ("H", 0, 2), ("K", 3, 1),
    ("G", 4, 3), ("D", 1, 0), ("G", 6, 3), ("H", 4, 1), ("K", 7, 1), ("H", 2, 2), ("G", 7, 1), ("G", 7, 2),
    ("K", 7, 2), ("H", 6, 1), ("D", 2, 0), ("K", 3, 3), ("H", 4, 2), ("G", 5, 3), ("H", 6, 2), ("K", 5, 3),
    ("D", 5, 0), ("H", 1, 3), ("G", 3, 3), ("G", 7, 3), ("H", 0, 3), ("K", 7, 3), ("H", 2, 3), ("H", 4, 3),
    ("D", 6, 0), ("H", 6, 3), ("D", 3, 0),
)


def plan(Z):
    if 1 + max(s for _, _, s in TUNED) == Z:
        return BATCHES, TUNED
    units, parts = range(len(UNITS)), range(len(PARTS))
    order = [("C", u, None) for u in units]
    order += [("Y", q, None) for q in parts if PARTS[q][3] == "A"]
    for q in parts:
        order += [("Z", q, None), ("Z", q, Z - 1), ("F", q, 0)]
    for q in parts:
        order += [("G", q, None)]
        order += [("H", q, None)] if PARTS[q][4] == "A" else [("H", q, 0), ("K", q, None)]
    return ((0, 0, Z), (1, 0, Z - 1)), order + [("D", 0, 0), ("D", 1, 0)]


def offsets(sizes):
    return [sum(sizes[:i]) for i in range(len(sizes) + 1)]


def partial_product(tok, held, h, p, Z, at):
    blocks = 2 * 2
    depth = blocks * held.shape[1]
    if len(tok.shape) == 3:
        left = tok[p, at, :]
    else:
        left = tok[at, pl.ds(pl.multiple_of(p * depth, depth), depth)]
    right = held[pl.ds((h * Z + p) * blocks, blocks)].reshape(depth, held.shape[2])
    return jnp.dot(left, right, preferred_element_type=F32)


def near_step(z, s, Z):
    m = jnp.minimum(z, Z - 1 - z)
    half = (s + 1) // 2 if isinstance(s, int) else lax.div(s + 1, 2)
    side = 2 * (s % 2) - 1 if isinstance(s, int) else 2 * lax.rem(s, 2) - 1
    place = jnp.where(s <= 2 * m, m + half * side, s)
    return jnp.where(2 * z >= Z, Z - 1 - place, place)


def kernel(
    Z,
    Y,
    replicas,
    tokens,
    pseudo_keys,
    pseudo_values,
    master_keys,
    moment_keys,
    master_values,
    moment_values,
    hyper_in,
    evals,
    states,
    tok,
    values,
    totals,
    mine,
    from_core,
    to_y,
    from_y,
    to_z,
    from_left,
    from_right,
    weights,
    total,
    acc,
    master,
    moment,
    hyper,
    load_sem,
    state_sem,
    tok_sem,
    rc_s,
    rc_r,
    sends,
    ry_r,
    z_r,
    gy_r,
    gc_r,
):
    me = lax.axis_index("replica")
    core = lax.rem(me, 2)
    chip = lax.div(me, 2)
    y = lax.rem(chip, Y)
    z = lax.div(chip, Y)
    oc = 1 - core
    oy = 1 - y

    def dev(zz, yy, cc):
        return {"replica": (zz * Y + yy) * 2 + cc}

    pseudo = (pseudo_keys, pseudo_values)
    units = len(UNITS)
    rows, cols = mine.shape[3:]
    count = acc.shape[1]
    batches, order = plan(Z)

    def lanes(u):
        return pl.ds(UNITS[u][1] * cols, cols)

    def edge(eighths):
        return rows if eighths == 8 else rows * eighths // 8 // 16 * 16

    spans = [pl.ds(edge(first), edge(last) - edge(first)) for _, first, last, _, _ in PARTS]
    unit = [part[0] for part in PARTS]
    reduce = [part[3] for part in PARTS]
    gather = [part[4] for part in PARTS]
    used = [q for q in range(len(PARTS)) if spans[q].size]

    loads = [
        pltpu.make_async_copy(
            pseudo[kv].at[:, :, core, :, lanes(u)], mine.at[u], load_sem.at[u]
        )
        for u, (kv, _) in enumerate(UNITS)
    ]
    state_loads = [
        pltpu.make_async_copy(src, dst, state_sem.at[i])
        for i, (src, dst) in enumerate(
            (
                (master_keys, master.at[0]),
                (moment_keys, moment.at[0]),
                (master_values, master.at[1]),
                (moment_values, moment.at[1]),
                (hyper_in, hyper),
            )
        )
    ]
    tok_load = pltpu.make_async_copy(tokens, tok, tok_sem)

    reduce_y_at = offsets([Z if kind == "A" else 1 for kind in reduce])
    gather_y_at = offsets([Z if kind == "A" else 1 for kind in gather])
    second_at = offsets([1 if kind == "A" else Z for kind in gather])

    def near(s):
        return near_step(z, s, Z)

    def far(s):
        return near(Z - 1 - s)

    def remote(src, dst, send, recv, device):
        return pltpu.make_async_remote_copy(
            src_ref=src,
            dst_ref=dst,
            send_sem=send,
            recv_sem=recv,
            device_id=device,
            device_id_type=MESH,
        )

    def core_copy(u, p):
        return remote(
            pseudo[UNITS[u][0]].at[p, :, oc, :, lanes(u)],
            from_core.at[u, p],
            rc_s,
            rc_r.at[u, p],
            dev(z, y, oc),
        )

    def y_copy(q, p):
        index = (unit[q], p, spans[q])
        slot = reduce_y_at[q] + (p if reduce[q] == "A" else 0)
        return remote(
            to_y.at[index], from_y.at[index], sends.at[q], ry_r.at[slot], dev(z, oy, core)
        )

    def second(q, p):
        return len(PARTS) * Z + second_at[q] + (p if gather[q] == "B" else 0)

    def z_refs(q, p):
        index = (unit[q], p, 0 if reduce[q] == "A" else slice(None), spans[q])
        return to_z.at[index], from_left.at[index], from_right.at[index]

    def right_copy(q, p):
        src, dst, _ = z_refs(q, p)
        return remote(src, dst, sends.at[q], z_r.at[q * Z + p], dev(z + 1, y, core))

    def left_copy(q, p, to):
        src, _, dst = z_refs(q, p)
        slot = jnp.where(p == to, second(q, p), q * Z + p)
        return remote(src, dst, sends.at[q], z_r.at[slot], dev(z - 1, y, core))

    def block(q, p, yy, cc):
        kv, h = UNITS[unit[q]]
        held = values if kv else weights
        return held.at[((h * Z + p) * Y + yy) * 2 + cc, spans[q]]

    def w_z(q, p, col, zz):
        w = block(q, p, oy if col else y, core)
        slot = second(q, p) if col else q * Z + p
        return remote(w, w, sends.at[q], z_r.at[slot], dev(zz, y, core))

    def w_y(q, p, yy):
        w = block(q, p, yy, core)
        slot = gather_y_at[q] + (p if gather[q] == "A" else 0)
        return remote(w, w, sends.at[q], gy_r.at[slot], dev(z, oy, core))

    def w_core(q, p, yy):
        w = block(q, p, yy, core)
        return remote(w, w, sends.at[q], gc_r.at[UNITS[unit[q]][0] * Z + p], dev(z, y, oc))

    def each(first, last, body):
        def run(s, carry):
            body(s)
            return carry

        lax.fori_loop(first, last, run, 0)

    for copy in loads:
        copy.start()

    @functools.partial(each, 0, count // 128)
    def _(i):
        at = pl.ds(pl.multiple_of(i * 128, 128), 128)
        for h in range(units // 2):
            acc[h, at, :] = jnp.zeros((128, cols), F32)
            totals[h, at, :] = jnp.zeros((128, cols), F32)

    barrier = pltpu.get_barrier_semaphore()
    pl.semaphore_signal(barrier, inc=1, device_id=dev(z, y, oc), device_id_type=MESH)
    pl.semaphore_signal(barrier, inc=1, device_id=dev(z, oy, core), device_id_type=MESH)

    @pl.when(z > 0)
    def _():
        pl.semaphore_signal(barrier, inc=1, device_id=dev(z - 1, y, core), device_id_type=MESH)

    @pl.when(z < Z - 1)
    def _():
        pl.semaphore_signal(barrier, inc=1, device_id=dev(z + 1, y, core), device_id_type=MESH)

    peers = 2 + jnp.where(z > 0, 1, 0) + jnp.where(z < Z - 1, 1, 0)
    pl.semaphore_wait(barrier, peers)

    for u in range(units):
        each(0, Z, lambda s: core_copy(u, far(s)).start())
    for copy in state_loads + [tok_load]:
        copy.start()

    loaded = set()

    def once(name, copy):
        if name not in loaded:
            loaded.add(name)
            copy.wait()

    def pair_sum(q, p, yy):
        index = (unit[q], p, yy, spans[q])
        return mine[index].astype(F32) + from_core[index].astype(F32)

    def reduce_y(q, s):
        p = far(s)
        to_y[unit[q], p, spans[q]] = pair_sum(q, p, oy).astype(BF16)
        y_copy(q, p).start()

    def reduce_z(q, s, last):
        p = far(s)
        u = unit[q]
        first = reduce[q] == "A"
        if first:
            y_copy(q, p).wait_recv()
            part = total.at[u, y, spans[q]]
            part[...] = pair_sum(q, p, y) + from_y[u, p, spans[q]].astype(F32)
        else:
            part = total.at[u, :, spans[q]]
            part[...] = pair_sum(q, p, slice(None))
        out, left, right = z_refs(q, p)

        @pl.when((p >= z) & (z > 0))
        def _():
            right_copy(q, p).wait_recv()
            part[...] += left[...].astype(F32)

        @pl.when((p <= z) & (z < Z - 1))
        def _():
            left_copy(q, p, z).wait_recv()
            part[...] += right[...].astype(F32)

        if not last:
            out[...] = part[...].astype(BF16)

            @pl.when(p > z)
            def _():
                right_copy(q, p).start()

            @pl.when(p < z)
            def _():
                left_copy(q, p, z - 1).start()
        elif not first:
            to_y[u, z, spans[q]] = total[u, oy, spans[q]].astype(BF16)
            y_copy(q, z).start()

    def spread(q, p, col):
        @pl.when((p < z) & (z < Z - 1))
        def _():
            w_z(q, p, col, z + 1).start()

        @pl.when((p > z) & (z > 0))
        def _():
            w_z(q, p, col, z - 1).start()

    def spread_own(q, col):
        @pl.when(z < Z - 1)
        def _():
            w_z(q, z, col, z + 1).start()

        @pl.when(z > 0)
        def _():
            w_z(q, z, col, z - 1).start()

    def update(q):
        u, span = unit[q], spans[q]
        kv, lane = UNITS[u][0], lanes(u)
        summed = total[u, y, span]
        if reduce[q] == "B":
            y_copy(q, z).wait_recv()
            summed += from_y[u, z, span].astype(F32)
        for i in (4, 2 * kv, 2 * kv + 1):
            once(("state", i), state_loads[i])
        outer_rate = hyper[0]
        outer_mom = hyper[1]
        averaged = summed / replicas
        moment_new = outer_mom * moment[kv, span, lane] + averaged
        master_new = master[kv, span, lane] - outer_rate * (averaged + outer_mom * moment_new)
        block(q, z, y, core)[...] = master_new.astype(BF16)
        if gather[q] == "A":
            spread_own(q, 0)
            w_y(q, z, y).start()
        else:
            w_y(q, z, y).start()
            spread_own(q, 0)
        w_core(q, z, y).start()
        states[2 * kv, span, lane] = master_new
        states[2 * kv + 1, span, lane] = moment_new

    def pass_z(q, s, col):
        p = near(s)
        w_z(q, p, col, z).wait_recv()
        spread(q, p, col)
        if gather[q] == "A":
            w_y(q, p, y).start()
        w_core(q, p, oy if col else y).start()

    def pass_y(q, s):
        p = near(s)
        w_y(q, p, oy).wait_recv()
        if gather[q] == "B":
            spread_own(q, 1)
        w_core(q, p, oy).start()

    tile = min(1024, count)

    def arrived(kv, p):
        w = weights.at[: units // 2 * Y] if kv == 0 else values.at[: units // 2 * Y]
        remote(w, w, rc_s, gc_r.at[kv * Z + p], dev(z, y, oc)).wait_recv()

    def products(kv, s0, s1):
        def one(t):
            p = near(s0 + t)
            arrived(kv, p)

            def strip(i):
                at = pl.ds(i * tile if isinstance(i, int) else pl.multiple_of(i * tile, tile), tile)
                for h in range(units // 2):
                    part = product(h, p, at, kv)
                    if kv:
                        totals[h, at, :] = part
                    else:
                        acc[h, at, :] = part
                        evals[at, h * cols : (h + 1) * cols] = part.astype(BF16)

            if count == tile:
                strip(0)
            else:
                each(0, count // tile, strip)

        each(0, s1 - s0, one)

    def product(h, p, at, kv):
        sums, held = (totals, values) if kv else (acc, weights)
        return sums[h, at, :] + partial_product(tok, held, h, p, Z, at)

    def drain():
        remote(from_core, from_core, rc_s, rc_s, dev(z, y, oc)).wait_send()

        def sent(q, blocks):
            w = weights.at[:blocks, spans[q]]
            remote(w, w, sends.at[q], sends.at[q], dev(z, y, oc)).wait_send()

        for inner in (True, False):

            @pl.when(((z > 0) & (z < Z - 1)) == inner)
            def _():
                for q in used:
                    beside = Z + 1 if inner else 1
                    across = beside + Z if gather[q] == "A" else 2 * beside + 1
                    sent(q, 2 * Z - 1 + across + 2 * Z)

    def take(kind, i, s):
        if kind == "C":
            once(i, loads[i])
            if s is None:
                each(0, Z, lambda t: core_copy(i, far(t)).wait_recv())
            else:
                core_copy(i, far(s)).wait_recv()
        elif kind == "Y":
            if s is None:
                each(0, Z, lambda t: reduce_y(i, t))
            else:
                reduce_y(i, s)
        elif kind == "Z":
            if s is None:
                each(0, Z - 1, lambda t: reduce_z(i, t, False))
            else:
                reduce_z(i, s, s == Z - 1)
        elif kind == "F":
            update(i)
        elif kind in ("G", "K"):
            col = 0 if kind == "G" else 1
            if s is None:
                each(1, Z, lambda t: pass_z(i, t, col))
            else:
                pass_z(i, s, col)
        elif kind == "H":
            if s is None:
                each(0, Z, lambda t: pass_y(i, t))
            else:
                pass_y(i, s)
        else:
            once("tokens", tok_load)
            products(*batches[i])

    for kind, i, s in order:
        if kind in "CD" or i in used:
            take(kind, i, s)
    arrived(1, near(Z - 1))
    drain()


def place(Z, Y, evals, states, tok, values, totals, *refs):
    target, result, sem = refs[:6], refs[6], refs[7]
    tile = min(512, result.shape[0])
    cols = values.shape[2]
    stores = [pltpu.make_async_copy(evals, target[0], sem.at[0])]
    stores += [
        pltpu.make_async_copy(states.at[i], target[2 + i], sem.at[1 + i]) for i in range(4)
    ]
    for copy in stores:
        copy.start()
    p = near_step(lax.div(lax.axis_index("replica"), 2 * Y), Z - 1, Z)
    for i in range(result.shape[0] // tile):
        at = pl.ds(i * tile, tile)
        for h in range(totals.shape[0]):
            part = totals[h, at, :] + partial_product(tok, values, h, p, Z, at)
            result[at, h * cols : (h + 1) * cols] = part.astype(BF16)
        copy = pltpu.make_async_copy(result.at[at], target[1].at[at], sem.at[5 + i])
        copy.start()
        stores.append(copy)
    for copy in stores:
        copy.wait()


def body(
    tokens,
    pseudo_keys,
    pseudo_values,
    master_keys,
    moment_keys,
    master_values,
    moment_values,
    outer_hyper,
):
    replicas = lax.axis_size("replica")
    Y = 2
    Z = replicas // (2 * Y)
    width = master_keys.shape[1]
    rows = master_keys.shape[0]
    count = tokens.shape[0]
    units = len(UNITS)
    halves = units // 2
    parts = len(PARTS)
    cols = 2 * width // units
    depth = 2 * Y * rows
    if depth % 128:
        tokens = tokens.reshape(count, Z, depth).swapaxes(0, 1)
    pseudo_keys, pseudo_values = (
        p.reshape(Z, Y, 2, rows, width) for p in (pseudo_keys, pseudo_values)
    )
    hbm = pl.BlockSpec(memory_space=pltpu.HBM)
    vmem = pl.BlockSpec(memory_space=pltpu.VMEM)
    dma = pltpu.SemaphoreType.DMA
    state = (master_keys.shape, F32)
    evaluated = ((count, width), BF16)
    shapes = (evaluated, evaluated, state, state, state, state)
    single = pltpu.VMEM((units, Z, rows, cols), BF16)
    double = pltpu.VMEM((units, Z, Y, rows, cols), BF16)
    results = pl.pallas_call(
        functools.partial(kernel, Z, Y, replicas),
        out_shape=(
            pltpu.VMEM((count, width), BF16),
            pltpu.VMEM((4, rows, width), F32),
            pltpu.VMEM(tokens.shape, BF16),
            pltpu.VMEM((halves * Z * Y * 2, rows, cols), BF16),
            pltpu.VMEM((halves, count, cols), F32),
        ),
        in_specs=[hbm] * 8,
        out_specs=(vmem,) * 5,
        scratch_shapes=[
            double,
            double,
            single,
            single,
            double,
            double,
            double,
            pltpu.VMEM((halves * Z * Y * 2, rows, cols), BF16),
            pltpu.VMEM((units, Y, rows, cols), F32),
            pltpu.VMEM((halves, count, cols), F32),
            pltpu.VMEM((2, rows, width), F32),
            pltpu.VMEM((2, rows, width), F32),
            pltpu.SMEM((2,), F32),
            dma((units,)),
            dma((5,)),
            dma,
            dma,
            dma((units, Z)),
            dma((parts,)),
            dma((sum(Z if part[3] == "A" else 1 for part in PARTS),)),
            dma((parts * Z + sum(1 if part[4] == "A" else Z for part in PARTS),)),
            dma((sum(Z if part[4] == "A" else 1 for part in PARTS),)),
            dma((2 * Z,)),
        ],
        compiler_params=pltpu.CompilerParams(
            collective_id=0, has_side_effects=True, vmem_limit_bytes=30 * 1024 * 1024
        ),
        name="outer_step",
    )(
        *[
            pltpu.with_memory_space_constraint(a, pltpu.HBM)
            for a in (
                tokens,
                pseudo_keys,
                pseudo_values,
                master_keys,
                moment_keys,
                master_values,
                moment_values,
                outer_hyper,
            )
        ]
    )
    return pl.pallas_call(
        functools.partial(place, Z, Y),
        out_shape=tuple(jax.ShapeDtypeStruct(*a) for a in shapes),
        in_specs=[vmem] * 5,
        out_specs=(hbm,) * 6,
        scratch_shapes=[
            pltpu.VMEM((count, width), BF16),
            dma((5 + count // min(512, count),)),
        ],
        compiler_params=pltpu.CompilerParams(vmem_limit_bytes=14 * 1024 * 1024),
        name="place",
    )(*[pltpu.with_memory_space_constraint(r, pltpu.VMEM) for r in results])


def solution(mesh):
    rows = P(("groups", "replica"), None)
    stack = P(("groups", "replica"), None, None)
    return jax.shard_map(
        body,
        mesh=mesh,
        in_specs=(rows, stack, stack, rows, rows, rows, rows, P("groups")),
        out_specs=(rows,) * 6,
        check_vma=False,
    )
```

```python
import functools

import jax
import jax.numpy as jnp
from jax import lax
from jax.experimental import pallas as pl
from jax.experimental.pallas import tpu as pltpu
from jax.sharding import PartitionSpec as P

MESH = pl.DeviceIdType.MESH
F32 = jnp.float32
BF16 = jnp.bfloat16

UNITS = ((0, 0), (0, 1), (1, 0), (1, 1))
PARTS = (
    (0, 0, 3, "A", "A"),
    (0, 3, 6, "A", "A"),
    (0, 6, 8, "B", "A"),
    (1, 0, 4, "A", "A"),
    (1, 4, 6, "A", "A"),
    (1, 6, 8, "B", "B"),
    (2, 0, 4, "A", "A"),
    (2, 4, 6, "A", "A"),
    (2, 6, 8, "B", "B"),
    (3, 0, 3, "A", "A"),
    (3, 3, 6, "A", "A"),
    (3, 6, 8, "B", "B"),
)

BATCHES = ((0, 0, 1), (0, 1, 2), (0, 2, 3), (0, 3, 4), (1, 0, 1), (1, 1, 2), (1, 2, 3), (1, 3, 4))
TUNED = (
    ("C", 0, 0), ("Y", 1, 0), ("Y", 0, 0), ("C", 0, 1), ("Y", 1, 1), ("Y", 0, 1), ("C", 0, 2), ("Y", 0, 2),
    ("Y", 1, 2), ("Z", 2, 0), ("C", 1, 0), ("Y", 4, 0), ("Y", 3, 0), ("Z", 5, 0), ("C", 2, 0), ("Y", 7, 0),
    ("Y", 6, 0), ("Z", 8, 0), ("C", 3, 0), ("Y", 10, 0), ("Y", 9, 0), ("C", 2, 1), ("Y", 6, 1), ("Z", 11, 0),
    ("Z", 2, 1), ("C", 2, 2), ("Y", 7, 2), ("Y", 7, 1), ("C", 0, 3), ("Y", 1, 3), ("C", 1, 3), ("Y", 4, 3),
    ("C", 1, 1), ("Y", 4, 1), ("C", 3, 1), ("Y", 9, 1), ("Z", 0, 0), ("Z", 5, 1), ("C", 1, 2), ("Z", 5, 2),
    ("C", 3, 2), ("Y", 9, 2), ("C", 2, 3), ("Y", 7, 3), ("Z", 1, 0), ("Y", 3, 1), ("Z", 4, 0), ("Y", 10, 1),
    ("Y", 4, 2), ("Z", 3, 0), ("Y", 3, 3), ("Z", 7, 0), ("Z", 6, 0), ("Z", 10, 0), ("Z", 9, 0), ("Z", 1, 1),
    ("Z", 0, 1), ("Y", 3, 2), ("Z", 8, 1), ("Z", 5, 3), ("Y", 0, 3), ("Z", 2, 2), ("Z", 4, 1), ("Y", 6, 3),
    ("Y", 10, 2), ("Z", 11, 1), ("Z", 0, 2), ("Z", 7, 1), ("Z", 1, 2), ("Z", 3, 1), ("Z", 8, 2), ("Z", 4, 2),
    ("Z", 11, 2), ("C", 3, 3), ("Y", 10, 3), ("Z", 2, 3), ("Z", 6, 1), ("Y", 6, 2), ("Z", 7, 2), ("Z", 9, 1),
    ("F", 5, 0), ("Z", 1, 3), ("F", 1, 0), ("Z", 10, 1), ("Z", 0, 3), ("Z", 3, 2), ("Z", 8, 3), ("F", 0, 0),
    ("Z", 4, 3), ("F", 4, 0), ("F", 2, 0), ("Z", 11, 3), ("G", 5, 1), ("Z", 6, 2), ("G", 1, 1), ("Z", 7, 3),
    ("H", 5, 0), ("F", 7, 0), ("Y", 9, 3), ("Z", 9, 2), ("F", 8, 0), ("G", 4, 1), ("G", 0, 1), ("Z", 10, 2),
    ("G", 2, 1), ("F", 11, 0), ("Z", 3, 3), ("F", 3, 0), ("K", 5, 1), ("G", 7, 1), ("H", 1, 0), ("G", 1, 2),
    ("H", 8, 0), ("G", 8, 1), ("Z", 6, 3), ("F", 6, 0), ("G", 4, 2), ("G", 0, 2), ("G", 11, 1), ("H", 4, 1),
    ("G", 3, 1), ("Z", 9, 3), ("F", 9, 0), ("H", 2, 0), ("Z", 10, 3), ("F", 10, 0), ("H", 2, 1), ("H", 1, 1),
    ("G", 2, 2), ("G", 7, 2), ("G", 6, 1), ("H", 11, 0), ("K", 8, 1), ("G", 3, 2), ("H", 0, 2), ("H", 7, 0),
    ("G", 9, 1), ("H", 4, 2), ("G", 6, 2), ("H", 0, 0), ("G", 10, 1), ("G", 9, 2), ("H", 4, 0), ("H", 0, 1),
    ("G", 10, 2), ("G", 1, 3), ("G", 5, 2), ("H", 3, 1), ("H", 9, 0), ("H", 3, 0), ("G", 2, 3), ("K", 8, 2),
    ("H", 6, 0), ("G", 0, 3), ("G", 4, 3), ("H", 10, 0), ("D", 0, 0), ("G", 3, 3), ("H", 2, 2), ("H", 7, 1),
    ("G", 11, 2), ("G", 8, 2), ("K", 5, 2), ("H", 1, 2), ("G", 7, 3), ("D", 4, 0), ("G", 6, 3), ("H", 7, 2),
    ("H", 3, 2), ("G", 9, 3), ("D", 1, 0), ("G", 10, 3), ("H", 6, 1), ("K", 11, 2), ("H", 9, 1),
    ("K", 11, 1), ("H", 6, 2), ("H", 10, 1), ("D", 2, 0), ("G", 5, 3), ("G", 8, 3), ("H", 9, 2),
    ("H", 10, 2), ("K", 8, 3), ("D", 5, 0), ("K", 5, 3), ("H", 2, 3), ("H", 1, 3), ("G", 11, 3), ("H", 0, 3),
    ("K", 11, 3), ("H", 4, 3), ("H", 6, 3), ("H", 7, 3), ("H", 3, 3), ("D", 6, 0), ("H", 9, 3), ("H", 10, 3),
    ("D", 3, 0),
)


def plan(Z):
    if 1 + max(s for _, _, s in TUNED) == Z:
        return BATCHES, TUNED
    units, parts = range(len(UNITS)), range(len(PARTS))
    order = [("C", u, None) for u in units]
    order += [("Y", q, None) for q in parts if PARTS[q][3] == "A"]
    for q in parts:
        order += [("Z", q, None), ("Z", q, Z - 1), ("F", q, 0)]
    for q in parts:
        order += [("G", q, None)]
        order += [("H", q, None)] if PARTS[q][4] == "A" else [("H", q, 0), ("K", q, None)]
    return ((0, 0, Z), (1, 0, Z - 1)), order + [("D", 0, 0), ("D", 1, 0)]


def offsets(sizes):
    return [sum(sizes[:i]) for i in range(len(sizes) + 1)]


def partial_product(tok, held, h, p, Z, at):
    blocks = 2 * 2
    depth = blocks * held.shape[1]
    if len(tok.shape) == 3:
        left = tok[p, at, :]
    else:
        left = tok[at, pl.ds(pl.multiple_of(p * depth, depth), depth)]
    right = held[pl.ds((h * Z + p) * blocks, blocks)].reshape(depth, held.shape[2])
    return jnp.dot(left, right, preferred_element_type=F32)


def near_step(z, s, Z):
    m = jnp.minimum(z, Z - 1 - z)
    half = (s + 1) // 2 if isinstance(s, int) else lax.div(s + 1, 2)
    side = 2 * (s % 2) - 1 if isinstance(s, int) else 2 * lax.rem(s, 2) - 1
    place = jnp.where(s <= 2 * m, m + half * side, s)
    return jnp.where(2 * z >= Z, Z - 1 - place, place)


def kernel(
    Z,
    Y,
    replicas,
    tokens,
    pseudo_keys,
    pseudo_values,
    master_keys,
    moment_keys,
    master_values,
    moment_values,
    hyper_in,
    evals,
    states,
    tok,
    values,
    totals,
    mine,
    from_core,
    to_y,
    from_y,
    to_z,
    from_left,
    from_right,
    weights,
    total,
    acc,
    master,
    moment,
    hyper,
    load_sem,
    state_sem,
    tok_sem,
    rc_s,
    rc_r,
    sends,
    ry_r,
    z_r,
    gy_r,
    gc_r,
):
    me = lax.axis_index("replica")
    core = lax.rem(me, 2)
    chip = lax.div(me, 2)
    y = lax.rem(chip, Y)
    z = lax.div(chip, Y)
    oc = 1 - core
    oy = 1 - y

    def dev(zz, yy, cc):
        return {"replica": (zz * Y + yy) * 2 + cc}

    pseudo = (pseudo_keys, pseudo_values)
    units = len(UNITS)
    rows, cols = mine.shape[3:]
    count = acc.shape[1]
    batches, order = plan(Z)

    def lanes(u):
        return pl.ds(UNITS[u][1] * cols, cols)

    def edge(eighths):
        return rows if eighths == 8 else rows * eighths // 8 // 16 * 16

    spans = [pl.ds(edge(first), edge(last) - edge(first)) for _, first, last, _, _ in PARTS]
    unit = [part[0] for part in PARTS]
    reduce = [part[3] for part in PARTS]
    gather = [part[4] for part in PARTS]
    used = [q for q in range(len(PARTS)) if spans[q].size]

    loads = [
        pltpu.make_async_copy(
            pseudo[kv].at[:, :, core, :, lanes(u)], mine.at[u], load_sem.at[u]
        )
        for u, (kv, _) in enumerate(UNITS)
    ]
    state_loads = [
        pltpu.make_async_copy(src, dst, state_sem.at[i])
        for i, (src, dst) in enumerate(
            (
                (master_keys, master.at[0]),
                (moment_keys, moment.at[0]),
                (master_values, master.at[1]),
                (moment_values, moment.at[1]),
                (hyper_in, hyper),
            )
        )
    ]
    tok_load = pltpu.make_async_copy(tokens, tok, tok_sem)

    reduce_y_at = offsets([Z if kind == "A" else 1 for kind in reduce])
    gather_y_at = offsets([Z if kind == "A" else 1 for kind in gather])
    second_at = offsets([1 if kind == "A" else Z for kind in gather])

    def near(s):
        return near_step(z, s, Z)

    def far(s):
        return near(Z - 1 - s)

    def remote(src, dst, send, recv, device):
        return pltpu.make_async_remote_copy(
            src_ref=src,
            dst_ref=dst,
            send_sem=send,
            recv_sem=recv,
            device_id=device,
            device_id_type=MESH,
        )

    def core_copy(u, p):
        return remote(
            pseudo[UNITS[u][0]].at[p, :, oc, :, lanes(u)],
            from_core.at[u, p],
            rc_s,
            rc_r.at[u, p],
            dev(z, y, oc),
        )

    def y_copy(q, p):
        index = (unit[q], p, spans[q])
        slot = reduce_y_at[q] + (p if reduce[q] == "A" else 0)
        return remote(
            to_y.at[index], from_y.at[index], sends.at[q], ry_r.at[slot], dev(z, oy, core)
        )

    def second(q, p):
        return len(PARTS) * Z + second_at[q] + (p if gather[q] == "B" else 0)

    def z_refs(q, p):
        index = (unit[q], p, 0 if reduce[q] == "A" else slice(None), spans[q])
        return to_z.at[index], from_left.at[index], from_right.at[index]

    def right_copy(q, p):
        src, dst, _ = z_refs(q, p)
        return remote(src, dst, sends.at[q], z_r.at[q * Z + p], dev(z + 1, y, core))

    def left_copy(q, p, to):
        src, _, dst = z_refs(q, p)
        slot = jnp.where(p == to, second(q, p), q * Z + p)
        return remote(src, dst, sends.at[q], z_r.at[slot], dev(z - 1, y, core))

    def block(q, p, yy, cc):
        kv, h = UNITS[unit[q]]
        held = values if kv else weights
        return held.at[((h * Z + p) * Y + yy) * 2 + cc, spans[q]]

    def w_z(q, p, col, zz):
        w = block(q, p, oy if col else y, core)
        slot = second(q, p) if col else q * Z + p
        return remote(w, w, sends.at[q], z_r.at[slot], dev(zz, y, core))

    def w_y(q, p, yy):
        w = block(q, p, yy, core)
        slot = gather_y_at[q] + (p if gather[q] == "A" else 0)
        return remote(w, w, sends.at[q], gy_r.at[slot], dev(z, oy, core))

    def w_core(q, p, yy):
        w = block(q, p, yy, core)
        return remote(w, w, sends.at[q], gc_r.at[UNITS[unit[q]][0] * Z + p], dev(z, y, oc))

    def each(first, last, body):
        def run(s, carry):
            body(s)
            return carry

        lax.fori_loop(first, last, run, 0)

    for copy in loads:
        copy.start()

    @functools.partial(each, 0, count // 128)
    def _(i):
        at = pl.ds(pl.multiple_of(i * 128, 128), 128)
        for h in range(units // 2):
            acc[h, at, :] = jnp.zeros((128, cols), F32)
            totals[h, at, :] = jnp.zeros((128, cols), F32)

    barrier = pltpu.get_barrier_semaphore()
    pl.semaphore_signal(barrier, inc=1, device_id=dev(z, y, oc), device_id_type=MESH)
    pl.semaphore_signal(barrier, inc=1, device_id=dev(z, oy, core), device_id_type=MESH)

    @pl.when(z > 0)
    def _():
        pl.semaphore_signal(barrier, inc=1, device_id=dev(z - 1, y, core), device_id_type=MESH)

    @pl.when(z < Z - 1)
    def _():
        pl.semaphore_signal(barrier, inc=1, device_id=dev(z + 1, y, core), device_id_type=MESH)

    peers = 2 + jnp.where(z > 0, 1, 0) + jnp.where(z < Z - 1, 1, 0)
    pl.semaphore_wait(barrier, peers)

    for u in range(units):
        each(0, Z, lambda s: core_copy(u, far(s)).start())
    for copy in state_loads + [tok_load]:
        copy.start()

    loaded = set()

    def once(name, copy):
        if name not in loaded:
            loaded.add(name)
            copy.wait()

    def pair_sum(q, p, yy):
        index = (unit[q], p, yy, spans[q])
        return mine[index].astype(F32) + from_core[index].astype(F32)

    def reduce_y(q, s):
        p = far(s)
        to_y[unit[q], p, spans[q]] = pair_sum(q, p, oy).astype(BF16)
        y_copy(q, p).start()

    def reduce_z(q, s, last):
        p = far(s)
        u = unit[q]
        first = reduce[q] == "A"
        if first:
            y_copy(q, p).wait_recv()
            part = total.at[u, y, spans[q]]
            part[...] = pair_sum(q, p, y) + from_y[u, p, spans[q]].astype(F32)
        else:
            part = total.at[u, :, spans[q]]
            part[...] = pair_sum(q, p, slice(None))
        out, left, right = z_refs(q, p)

        @pl.when((p >= z) & (z > 0))
        def _():
            right_copy(q, p).wait_recv()
            part[...] += left[...].astype(F32)

        @pl.when((p <= z) & (z < Z - 1))
        def _():
            left_copy(q, p, z).wait_recv()
            part[...] += right[...].astype(F32)

        if not last:
            out[...] = part[...].astype(BF16)

            @pl.when(p > z)
            def _():
                right_copy(q, p).start()

            @pl.when(p < z)
            def _():
                left_copy(q, p, z - 1).start()
        elif not first:
            to_y[u, z, spans[q]] = total[u, oy, spans[q]].astype(BF16)
            y_copy(q, z).start()

    def spread(q, p, col):
        @pl.when((p < z) & (z < Z - 1))
        def _():
            w_z(q, p, col, z + 1).start()

        @pl.when((p > z) & (z > 0))
        def _():
            w_z(q, p, col, z - 1).start()

    def spread_own(q, col):
        @pl.when(z < Z - 1)
        def _():
            w_z(q, z, col, z + 1).start()

        @pl.when(z > 0)
        def _():
            w_z(q, z, col, z - 1).start()

    def update(q):
        u, span = unit[q], spans[q]
        kv, lane = UNITS[u][0], lanes(u)
        summed = total[u, y, span]
        if reduce[q] == "B":
            y_copy(q, z).wait_recv()
            summed += from_y[u, z, span].astype(F32)
        for i in (4, 2 * kv, 2 * kv + 1):
            once(("state", i), state_loads[i])
        outer_rate = hyper[0]
        outer_mom = hyper[1]
        averaged = summed / replicas
        moment_new = outer_mom * moment[kv, span, lane] + averaged
        master_new = master[kv, span, lane] - outer_rate * (averaged + outer_mom * moment_new)
        block(q, z, y, core)[...] = master_new.astype(BF16)
        if gather[q] == "A":
            spread_own(q, 0)
            w_y(q, z, y).start()
        else:
            w_y(q, z, y).start()
            spread_own(q, 0)
        w_core(q, z, y).start()
        states[2 * kv, span, lane] = master_new
        states[2 * kv + 1, span, lane] = moment_new

    def pass_z(q, s, col):
        p = near(s)
        w_z(q, p, col, z).wait_recv()
        spread(q, p, col)
        if gather[q] == "A":
            w_y(q, p, y).start()
        w_core(q, p, oy if col else y).start()

    def pass_y(q, s):
        p = near(s)
        w_y(q, p, oy).wait_recv()
        if gather[q] == "B":
            spread_own(q, 1)
        w_core(q, p, oy).start()

    tile = min(1024, count)

    def arrived(kv, p):
        w = weights.at[: units // 2 * Y] if kv == 0 else values.at[: units // 2 * Y]
        remote(w, w, rc_s, gc_r.at[kv * Z + p], dev(z, y, oc)).wait_recv()

    def products(kv, s0, s1):
        def one(t):
            p = near(s0 + t)
            arrived(kv, p)

            def strip(i):
                at = pl.ds(i * tile if isinstance(i, int) else pl.multiple_of(i * tile, tile), tile)
                for h in range(units // 2):
                    part = product(h, p, at, kv)
                    if kv:
                        totals[h, at, :] = part
                    else:
                        acc[h, at, :] = part
                        evals[at, h * cols : (h + 1) * cols] = part.astype(BF16)

            if count == tile:
                strip(0)
            else:
                each(0, count // tile, strip)

        each(0, s1 - s0, one)

    def product(h, p, at, kv):
        sums, held = (totals, values) if kv else (acc, weights)
        return sums[h, at, :] + partial_product(tok, held, h, p, Z, at)

    def drain():
        remote(from_core, from_core, rc_s, rc_s, dev(z, y, oc)).wait_send()

        def sent(q, blocks):
            w = weights.at[:blocks, spans[q]]
            remote(w, w, sends.at[q], sends.at[q], dev(z, y, oc)).wait_send()

        for inner in (True, False):

            @pl.when(((z > 0) & (z < Z - 1)) == inner)
            def _():
                for q in used:
                    beside = Z + 1 if inner else 1
                    across = beside + Z if gather[q] == "A" else 2 * beside + 1
                    sent(q, 2 * Z - 1 + across + 2 * Z)

    def take(kind, i, s):
        if kind == "C":
            once(i, loads[i])
            if s is None:
                each(0, Z, lambda t: core_copy(i, far(t)).wait_recv())
            else:
                core_copy(i, far(s)).wait_recv()
        elif kind == "Y":
            if s is None:
                each(0, Z, lambda t: reduce_y(i, t))
            else:
                reduce_y(i, s)
        elif kind == "Z":
            if s is None:
                each(0, Z - 1, lambda t: reduce_z(i, t, False))
            else:
                reduce_z(i, s, s == Z - 1)
        elif kind == "F":
            update(i)
        elif kind in ("G", "K"):
            col = 0 if kind == "G" else 1
            if s is None:
                each(1, Z, lambda t: pass_z(i, t, col))
            else:
                pass_z(i, s, col)
        elif kind == "H":
            if s is None:
                each(0, Z, lambda t: pass_y(i, t))
            else:
                pass_y(i, s)
        else:
            once("tokens", tok_load)
            products(*batches[i])

    for kind, i, s in order:
        if kind in "CD" or i in used:
            take(kind, i, s)
    arrived(1, near(Z - 1))
    drain()


def place(Z, Y, evals, states, tok, values, totals, *refs):
    target, result, sem = refs[:6], refs[6], refs[7]
    tile = min(512, result.shape[0])
    cols = values.shape[2]
    stores = [pltpu.make_async_copy(evals, target[0], sem.at[0])]
    stores += [
        pltpu.make_async_copy(states.at[i], target[2 + i], sem.at[1 + i]) for i in range(4)
    ]
    for copy in stores:
        copy.start()
    p = near_step(lax.div(lax.axis_index("replica"), 2 * Y), Z - 1, Z)
    for i in range(result.shape[0] // tile):
        at = pl.ds(i * tile, tile)
        for h in range(totals.shape[0]):
            part = totals[h, at, :] + partial_product(tok, values, h, p, Z, at)
            result[at, h * cols : (h + 1) * cols] = part.astype(BF16)
        copy = pltpu.make_async_copy(result.at[at], target[1].at[at], sem.at[5 + i])
        copy.start()
        stores.append(copy)
    for copy in stores:
        copy.wait()


def body(
    tokens,
    pseudo_keys,
    pseudo_values,
    master_keys,
    moment_keys,
    master_values,
    moment_values,
    outer_hyper,
):
    replicas = lax.axis_size("replica")
    Y = 2
    Z = replicas // (2 * Y)
    width = master_keys.shape[1]
    rows = master_keys.shape[0]
    count = tokens.shape[0]
    units = len(UNITS)
    halves = units // 2
    parts = len(PARTS)
    cols = 2 * width // units
    depth = 2 * Y * rows
    if depth % 128:
        tokens = tokens.reshape(count, Z, depth).swapaxes(0, 1)
    pseudo_keys, pseudo_values = (
        p.reshape(Z, Y, 2, rows, width) for p in (pseudo_keys, pseudo_values)
    )
    hbm = pl.BlockSpec(memory_space=pltpu.HBM)
    vmem = pl.BlockSpec(memory_space=pltpu.VMEM)
    dma = pltpu.SemaphoreType.DMA
    state = (master_keys.shape, F32)
    evaluated = ((count, width), BF16)
    shapes = (evaluated, evaluated, state, state, state, state)
    single = pltpu.VMEM((units, Z, rows, cols), BF16)
    double = pltpu.VMEM((units, Z, Y, rows, cols), BF16)
    results = pl.pallas_call(
        functools.partial(kernel, Z, Y, replicas),
        out_shape=(
            pltpu.VMEM((count, width), BF16),
            pltpu.VMEM((4, rows, width), F32),
            pltpu.VMEM(tokens.shape, BF16),
            pltpu.VMEM((halves * Z * Y * 2, rows, cols), BF16),
            pltpu.VMEM((halves, count, cols), F32),
        ),
        in_specs=[hbm] * 8,
        out_specs=(vmem,) * 5,
        scratch_shapes=[
            double,
            double,
            single,
            single,
            double,
            double,
            double,
            pltpu.VMEM((halves * Z * Y * 2, rows, cols), BF16),
            pltpu.VMEM((units, Y, rows, cols), F32),
            pltpu.VMEM((halves, count, cols), F32),
            pltpu.VMEM((2, rows, width), F32),
            pltpu.VMEM((2, rows, width), F32),
            pltpu.SMEM((2,), F32),
            dma((units,)),
            dma((5,)),
            dma,
            dma,
            dma((units, Z)),
            dma((parts,)),
            dma((sum(Z if part[3] == "A" else 1 for part in PARTS),)),
            dma((parts * Z + sum(1 if part[4] == "A" else Z for part in PARTS),)),
            dma((sum(Z if part[4] == "A" else 1 for part in PARTS),)),
            dma((2 * Z,)),
        ],
        compiler_params=pltpu.CompilerParams(
            collective_id=0, has_side_effects=True, vmem_limit_bytes=30 * 1024 * 1024
        ),
        name="outer_step",
    )(
        *[
            pltpu.with_memory_space_constraint(a, pltpu.HBM)
            for a in (
                tokens,
                pseudo_keys,
                pseudo_values,
                master_keys,
                moment_keys,
                master_values,
                moment_values,
                outer_hyper,
            )
        ]
    )
    return pl.pallas_call(
        functools.partial(place, Z, Y),
        out_shape=tuple(jax.ShapeDtypeStruct(*a) for a in shapes),
        in_specs=[vmem] * 5,
        out_specs=(hbm,) * 6,
        scratch_shapes=[
            pltpu.VMEM((count, width), BF16),
            dma((5 + count // min(512, count),)),
        ],
        compiler_params=pltpu.CompilerParams(vmem_limit_bytes=14 * 1024 * 1024),
        name="place",
    )(*[pltpu.with_memory_space_constraint(r, pltpu.VMEM) for r in results])


def solution(mesh):
    rows = P(("groups", "replica"), None)
    stack = P(("groups", "replica"), None, None)
    return jax.shard_map(
        body,
        mesh=mesh,
        in_specs=(rows, stack, stack, rows, rows, rows, rows, P("groups")),
        out_specs=(rows,) * 6,
        check_vma=False,
    )
```
